32 devices in a mesh: seq: 8 (over y, x, core), head: 4 (over z).
Axes of the slice: x: 2, y: 2, z: 4, core: 2. Of those that a mesh axis runs over, the one named last changes fastest.
Arguments:
- video_rows: bfloat16 [4096, 5120], P('seq'), may hold values from -6 to 6
- context: bfloat16 [512, 5120], P('seq'), may hold values from -6 to 6
- valid_length: int32 [1], replicated, may hold values from 64 to 512
- timestep: int32 [1], replicated, may hold values from 0 to 999
- query_weight: bfloat16 [5120, 1024], P('seq', 'head'), may hold values from -0.078125 to 0.078125
- key_weight: bfloat16 [5120, 1024], P('seq', 'head'), may hold values from -0.078125 to 0.078125
- value_weight: bfloat16 [5120, 1024], P('seq', 'head'), may hold values from -0.078125 to 0.078125
- out_weight: bfloat16 [1024, 5120], P('head', 'seq'), may hold values from -0.1875 to 0.1875
- query_gain: float32 [1024], P('head'), may hold values from 0.5 to 15
- key_gain: float32 [1024], P('head'), may hold values from 0.5 to 15
- time_weight: bfloat16 [2, 256, 5120], P(None, None, 'head'), may hold values from -0.375 to 0.375
- modulation: float32 [2, 5120], P(None, 'head'), may hold values from -3 to 3
Outputs:
- residual_out: bfloat16 [4096, 5120], P('seq', 'head')
- modulated: bfloat16 [4096, 5120], P('seq', 'head')
The draws below stay inside these ranges and needn't reach their ends.
Inputs may be any that keep to these rules, and one draw needn't show every extreme that they name: `valid_length`: text positions at or beyond it are padding.
All inputs are finite; a program needn't handle non-finite values.
Results may differ from the reference program's by a relative error of at most 0.0065.
The reference program's roundings to bfloat16 on the way (of `normed`, `value_proj`, `query_normed`, `key_normed`, `weights`, `attended` and `act`) count: a program that leaves them out, or rounds other values in their place, can miss the bound.
Values may be sent and summed in bfloat16 or wider, within the bound.
No kernel may reach another device: no remote copies, remote signals or barrier semaphores. Data moves between devices by JAX's collectives and lax.ppermute only.
A program may use at most 64 MiB of HBM per device.

```python
import jax
import jax.numpy as jnp
from jax import lax

D = 5120
HD = 128
TEXT = 512
FREQ = 256
HEADS = 8
ATT = 1024
TOKENS = 4096


def head_gains(key):
    base = jax.random.uniform(key, (HEADS, HD), jnp.float32, 0.5, 1.5)
    return base.reshape(HEADS * HD)


def draw_query_gain(key, part):
    return head_gains(jax.random.fold_in(key, 11))


def draw_key_gain(key, part):
    return head_gains(jax.random.fold_in(key, 23))


def shard_levels(rng, shape, cuts, least, top_value):
    def one(axis_at, parts):
        steps = jax.random.uniform(jax.random.fold_in(jax.random.fold_in(rng, 6), axis_at), (parts,), jnp.float32, least / len(cuts), top_value / len(cuts))
        return jnp.repeat(jnp.exp(steps), shape[axis_at] // parts).reshape((-1,) + (1,) * (len(shape) - axis_at - 1))

    loudness = one(*cuts[0])
    for cut in cuts[1:]:
        loudness = loudness * one(*cut)
    return loudness


def centred(own_key, shape, deviation, limit, pieces=(), held_as=jnp.bfloat16):
    loudness = shard_levels(own_key, shape, pieces, -0.22, 0.18) if pieces else 1.0
    entries = jax.random.normal(own_key, shape, jnp.float32) * deviation * loudness
    return jnp.minimum(jnp.maximum(entries, -limit), limit).astype(held_as)


def setup_inputs(seed: int = 0) -> dict:
    arg_keys = jax.random.split(jax.random.key(seed), 13)
    video_rows = centred(arg_keys[0], (TOKENS, D), 1.0, 6.0, ((0, 8),))
    context = centred(arg_keys[1], (TEXT, D), 1.0, 6.0, ((0, 8),))
    valid_length = jax.random.randint(arg_keys[2], (1,), TEXT // 8, TEXT + 1).astype(jnp.int32)
    timestep = jax.random.randint(arg_keys[3], (1,), 0, 1000).astype(jnp.int32)
    query_weight = centred(arg_keys[4], (D, ATT), D ** -0.5, 0.078125, ((0, 8), (1, 4)))
    key_weight = centred(arg_keys[5], (D, ATT), D ** -0.5, 0.078125, ((0, 8), (1, 4)))
    value_weight = centred(arg_keys[6], (D, ATT), D ** -0.5, 0.078125, ((0, 8), (1, 4)))
    out_weight = centred(arg_keys[7], (ATT, D), ATT ** -0.5, 0.1875, ((0, 4), (1, 8)))
    query_gain = draw_query_gain(jax.random.fold_in(arg_keys[12], 71), 0)
    key_gain = draw_key_gain(jax.random.fold_in(arg_keys[12], 71), 0)
    time_weight = centred(arg_keys[10], (2, FREQ, D), FREQ ** -0.5, 0.375, ((2, 4),))
    modulation = centred(arg_keys[11], (2, D), 0.5, 3.0, ((1, 4),), jnp.float32)
    return {"video_rows": video_rows, "context": context, "valid_length": valid_length, "timestep": timestep, "query_weight": query_weight, "key_weight": key_weight, "value_weight": value_weight, "out_weight": out_weight, "query_gain": query_gain, "key_gain": key_gain, "time_weight": time_weight, "modulation": modulation}


def layer_norm(rows):
    mean = lax.optimization_barrier(jnp.mean(rows, axis=-1, keepdims=True))
    spread = lax.optimization_barrier(jnp.mean((rows - mean) ** 2, axis=-1, keepdims=True))
    return (rows - mean) / jnp.sqrt(spread + 1e-06)

def rms_gain(rows, gain):
    return rows / jnp.sqrt(lax.optimization_barrier(jnp.mean(rows * rows, axis=-1, keepdims=True)) + 1e-06) * gain

def reference(video_rows, context, valid_length, timestep, query_weight, key_weight, value_weight, out_weight, query_gain, key_gain, time_weight, modulation):
    normed = layer_norm(video_rows.astype(jnp.float32)).astype(jnp.bfloat16)
    queries = jnp.dot(normed, query_weight, preferred_element_type=jnp.float32)
    key_proj = jnp.dot(context, key_weight, preferred_element_type=jnp.float32)
    value_proj = jnp.dot(context, value_weight, preferred_element_type=jnp.float32).astype(jnp.bfloat16)
    query_normed = rms_gain(queries, query_gain).astype(jnp.bfloat16)
    key_normed = rms_gain(key_proj, key_gain).astype(jnp.bfloat16)
    key_valid = jnp.arange(TEXT, dtype=jnp.int32) < valid_length[0]

    def one_head(head_index):
        offset = (head_index * HD).astype(jnp.int32)
        query_part = lax.dynamic_slice_in_dim(query_normed, offset, HD, 1)
        key_part = lax.dynamic_slice_in_dim(key_normed, offset, HD, 1)
        value_part = lax.dynamic_slice_in_dim(value_proj, offset, HD, 1)
        scores = jnp.dot(query_part, key_part.T, preferred_element_type=jnp.float32) * HD ** (-0.5)
        scores = jnp.where(key_valid[None, :], scores, jnp.float32(-1e+30))
        shifted = jnp.exp(scores - lax.optimization_barrier(jnp.max(scores, axis=-1, keepdims=True)))
        weights = (shifted / lax.optimization_barrier(jnp.sum(shifted, axis=-1, keepdims=True))).astype(jnp.bfloat16)
        return jnp.dot(weights, value_part, preferred_element_type=jnp.float32).astype(jnp.bfloat16)
    per_head = lax.map(one_head, jnp.arange(HEADS, dtype=jnp.int32))
    attended = jnp.transpose(per_head, (1, 0, 2)).reshape(TOKENS, ATT)
    projected = jnp.dot(attended, out_weight, preferred_element_type=jnp.float32)
    residual_out = (video_rows.astype(jnp.float32) + projected).astype(jnp.bfloat16)
    half = FREQ // 2
    freqs = jnp.exp(-jnp.log(10000.0) * jnp.arange(half, dtype=jnp.float32) / half)
    angles = timestep[0].astype(jnp.float32) * freqs
    embedding = jnp.concatenate([jnp.cos(angles), jnp.sin(angles)])
    act = jax.nn.silu(embedding).astype(jnp.bfloat16)[None, :]
    shift = modulation[0] + jnp.dot(act, time_weight[0], preferred_element_type=jnp.float32)[0]
    scale = modulation[1] + jnp.dot(act, time_weight[1], preferred_element_type=jnp.float32)[0]
    resid = residual_out.astype(jnp.float32)
    mean2 = lax.optimization_barrier(jnp.mean(resid, axis=-1, keepdims=True))
    var2 = lax.optimization_barrier(jnp.mean(resid * resid, axis=-1, keepdims=True)) - mean2 * mean2
    modulated = ((resid - mean2) / jnp.sqrt(var2 + 1e-06) * (1.0 + scale) + shift).astype(jnp.bfloat16)
    return (residual_out, modulated)
```

```python
import jax
import jax.numpy as jnp
from jax import lax
from jax.sharding import PartitionSpec as P

HD = 128
FREQ = 256


def dot32(left, right):
    return jnp.dot(left, right, preferred_element_type=jnp.float32)


class Layout:
    def __init__(self):
        self.seq = lax.axis_size("seq")
        self.head = lax.axis_size("head")
        self.mates = self.seq // self.head
        self.groups = self.seq // self.mates
        index = lax.axis_index("seq")
        self.group = index // self.mates
        self.mate = index % self.mates
        self.plane = lax.axis_index("head")

    def to_peer(self, x, k):
        if k == 0:
            return x
        pairs = [
            (g * self.mates + m, (g ^ k) * self.mates + m)
            for g in range(self.groups)
            for m in range(self.mates)
        ]
        return lax.ppermute(x, "seq", pairs)

    def to_mate(self, x, m):
        if m == 0:
            return x
        pairs = [(i, i ^ m) for i in range(self.seq)]
        return lax.ppermute(x, "seq", pairs)

    def to_plane(self, x, k):
        if k == 0:
            return x
        return lax.ppermute(x, "head", [(i, i ^ k) for i in range(self.head)])

    def block(self, k, m):
        return (self.group ^ k) * self.mates + (self.mate ^ m)

    def plane_sum(self, x):
        total = x
        for k in range(1, self.head):
            total = total + self.to_plane(x, k)
        return total


def take(x, index, size, axis):
    return lax.dynamic_slice_in_dim(x, index * size, size, axis)


def gather_out_weight(lay, out_weight):
    rows, cols = out_weight.shape
    piece = rows // lay.groups
    first = jnp.stack(
        [
            lay.to_peer(take(out_weight, lay.group ^ k, piece, 0), k)
            for k in range(lay.groups)
        ]
    )
    second = jnp.stack(
        [
            lay.to_plane(
                lax.dynamic_index_in_dim(first, lay.group ^ lay.plane ^ k, 0, False), k
            )
            for k in range(lay.head)
        ]
    )
    third = jnp.stack([lay.to_peer(second, k) for k in range(lay.groups)])
    halves = jnp.stack([lay.to_mate(third, m) for m in range(lay.mates)])
    columns = []
    for m in range(lay.mates):
        half = lax.dynamic_index_in_dim(halves, lay.mate ^ m, 0, False)
        pieces = [
            lax.dynamic_index_in_dim(half, lay.group ^ g, 0, False)
            for g in range(lay.groups)
        ]
        columns.append(jnp.concatenate(pieces, axis=1))
    return jnp.concatenate(columns, axis=2)


def project_text(lay, context, key_weight, value_weight, key_gain, total_att):
    depth, att = key_weight.shape
    text_local = context.shape[0]
    pair = jnp.concatenate([key_weight, value_weight], axis=1)
    weights = jnp.concatenate([lay.to_mate(pair, m) for m in range(lay.mates)], axis=0)
    rows = []
    for k in range(lay.groups):
        piece = jnp.concatenate(
            [take(context, lay.block(k, m), depth, 1) for m in range(lay.mates)], axis=1
        )
        rows.append(lay.to_peer(piece, k))
    partial = dot32(jnp.concatenate(rows, axis=0), weights)
    total = partial[:text_local]
    for k in range(1, lay.groups):
        total = total + lay.to_peer(partial[k * text_local : (k + 1) * text_local], k)
    keys, values = total[:, :att], total[:, att:]
    square = lay.plane_sum(jnp.sum(keys * keys, axis=1))
    keys = (keys / jnp.sqrt(square[:, None] / total_att + 1e-06) * key_gain).astype(
        jnp.bfloat16
    )
    packed = jnp.concatenate([keys, values.astype(jnp.bfloat16)], axis=1)
    packed = jnp.concatenate([lay.to_peer(packed, k) for k in range(lay.groups)], axis=0)
    packed = jnp.concatenate([lay.to_mate(packed, m) for m in range(lay.mates)], axis=0)
    places = jnp.concatenate(
        [
            lay.block(k, m) * text_local + jnp.arange(text_local, dtype=jnp.int32)
            for m in range(lay.mates)
            for k in range(lay.groups)
        ]
    )
    return packed[:, :att], packed[:, att:], places


def project_queries(lay, video_rows, query_weight, query_gain, total_att):
    depth = query_weight.shape[0]
    rows = video_rows.astype(jnp.float32)
    mean = jnp.mean(rows, axis=-1, keepdims=True)
    spread = jnp.mean((rows - mean) ** 2, axis=-1, keepdims=True)
    root = jnp.sqrt(spread + 1e-06)
    queries = None
    for k in range(lay.groups):
        mine = lay.to_peer(query_weight, k)
        for m in range(lay.mates):
            part = take(video_rows, lay.block(k, m), depth, 1).astype(jnp.float32)
            normed = ((part - mean) / root).astype(jnp.bfloat16)
            term = dot32(normed, lay.to_mate(mine, m))
            queries = term if queries is None else queries + term
    square = lay.plane_sum(jnp.sum(queries * queries, axis=1))
    return (queries / jnp.sqrt(square[:, None] / total_att + 1e-06) * query_gain).astype(
        jnp.bfloat16
    )


def attend(queries, keys, values, places, valid_length):
    tok_rows, local_att = queries.shape
    text_count = keys.shape[0]
    heads = local_att // HD
    key_valid = places < valid_length[0]
    scores = jnp.einsum(
        "thd,shd->hts",
        queries.reshape(tok_rows, heads, HD),
        keys.reshape(text_count, heads, HD),
        preferred_element_type=jnp.float32,
    ) * HD ** (-0.5)
    scores = jnp.where(key_valid[None, None, :], scores, jnp.float32(-1e30))
    shifted = jnp.exp(scores - jnp.max(scores, axis=-1, keepdims=True))
    weights = (shifted / jnp.sum(shifted, axis=-1, keepdims=True)).astype(jnp.bfloat16)
    attended = jnp.einsum(
        "hts,shd->thd",
        weights,
        values.reshape(text_count, heads, HD),
        preferred_element_type=jnp.float32,
    ).astype(jnp.bfloat16)
    return attended.reshape(tok_rows, local_att)


def shift_and_scale(timestep, time_weight, modulation):
    half = FREQ // 2
    freqs = jnp.exp(-jnp.log(10000.0) * jnp.arange(half, dtype=jnp.float32) / half)
    angles = timestep[0].astype(jnp.float32) * freqs
    embedding = jnp.concatenate([jnp.cos(angles), jnp.sin(angles)])
    act = jax.nn.silu(embedding).astype(jnp.bfloat16)[None, :]
    shift = modulation[0] + dot32(act, time_weight[0])[0]
    scale = modulation[1] + dot32(act, time_weight[1])[0]
    return shift, scale


def on_device(
    video_rows,
    context,
    valid_length,
    timestep,
    query_weight,
    key_weight,
    value_weight,
    out_weight,
    query_gain,
    key_gain,
    time_weight,
    modulation,
):
    lay = Layout()
    total_att = query_weight.shape[1] * lay.head
    width_local = modulation.shape[1]
    keys, values, places = project_text(
        lay, context, key_weight, value_weight, key_gain, total_att
    )
    queries = project_queries(lay, video_rows, query_weight, query_gain, total_att)
    block_rows = gather_out_weight(lay, out_weight)
    attended = attend(queries, keys, values, places, valid_length)
    projected = None
    for k in range(lay.head):
        term = dot32(lay.to_plane(attended, k), block_rows[k])
        projected = term if projected is None else projected + term
    video_part = take(video_rows, lay.plane, width_local, 1)
    residual_out = (video_part.astype(jnp.float32) + projected).astype(jnp.bfloat16)
    shift, scale = shift_and_scale(timestep, time_weight, modulation)
    resid = residual_out.astype(jnp.float32)
    sums = lay.plane_sum(jnp.stack([jnp.sum(resid, axis=1), jnp.sum(resid * resid, axis=1)]))
    full_width = width_local * lay.head
    mean2 = (sums[0] / full_width)[:, None]
    var2 = (sums[1] / full_width)[:, None] - mean2 * mean2
    modulated = ((resid - mean2) / jnp.sqrt(var2 + 1e-06) * (1.0 + scale) + shift).astype(
        jnp.bfloat16
    )
    return (residual_out, modulated)


def solution(mesh):
    in_specs = (
        P("seq", None),
        P("seq", None),
        P(),
        P(),
        P("seq", "head"),
        P("seq", "head"),
        P("seq", "head"),
        P("head", "seq"),
        P("head"),
        P("head"),
        P(None, None, "head"),
        P(None, "head"),
    )
    out_specs = (P("seq", "head"), P("seq", "head"))
    return jax.shard_map(
        on_device, mesh=mesh, in_specs=in_specs, out_specs=out_specs, check_vma=False
    )
```

```python
import functools

import jax
import jax.numpy as jnp
from jax import lax
from jax.experimental import pallas as pl
from jax.experimental.pallas import tpu as pltpu
from jax.sharding import PartitionSpec as P


HD = 128
FREQ = 256


def dot32(left, right):
    return jnp.dot(left, right, preferred_element_type=jnp.float32)


def take(x, index, size, axis):
    return lax.dynamic_slice_in_dim(x, index * size, size, axis)


def pick(x, index):
    return lax.dynamic_index_in_dim(x, index, 0, False)


class Layout:
    def __init__(self):
        self.seq = lax.axis_size("seq")
        self.head = lax.axis_size("head")
        self.mates = self.seq // self.head
        self.groups = self.seq // self.mates
        self.bits = self.groups.bit_length() - 1
        index = lax.axis_index("seq")
        self.group = index // self.mates
        self.mate = index % self.mates
        self.plane = lax.axis_index("head")

    def permute(self, x, axis, pairs):
        return lax.ppermute(x, axis, pairs)

    def to_peer(self, x, k):
        if k == 0:
            return x
        pairs = [
            (g * self.mates + m, (g ^ k) * self.mates + m)
            for g in range(self.groups)
            for m in range(self.mates)
        ]
        return self.permute(x, "seq", pairs)

    def to_mate(self, x, m):
        if m == 0:
            return x
        return self.permute(x, "seq", [(i, i ^ m) for i in range(self.seq)])

    def to_plane(self, x, k):
        if k == 0:
            return x
        return self.permute(x, "head", [(i, i ^ k) for i in range(self.head)])

    def turned(self, step, m):
        return 1 << ((step + m) % self.bits)

    def double(self, x):
        have = [x]
        for step in range(self.bits):
            pairs = [
                (g * self.mates + m, (g ^ self.turned(step, m)) * self.mates + m)
                for g in range(self.groups)
                for m in range(self.mates)
            ]
            whole = jnp.concatenate(have, axis=0) if step else x
            have.append(self.permute(whole, "seq", pairs))
        return have

    def to_mate_each(self, pieces, m):
        return [self.to_mate(x, m) for x in pieces]

    def mask(self, slot, mate):
        total = jnp.int32(0)
        for m in range(self.mates):
            value = 0
            for step in range(self.bits):
                if slot >> step & 1:
                    value |= self.turned(step, m)
            total = total + jnp.where(mate == m, value, 0)
        return total

    def plane_sum(self, x):
        total = x
        for k in range(1, self.head):
            total = total + self.to_plane(x, k)
        return total


def norm_kernel(order, rows_ref, out_ref):
    width = rows_ref.shape[1]
    count = order.shape[0]
    depth = width // count
    lanes = 128
    total = jnp.zeros((rows_ref.shape[0], lanes), jnp.float32)
    for c in range(width // lanes):
        total = total + rows_ref[:, c * lanes : (c + 1) * lanes].astype(jnp.float32)
    mean = jnp.sum(total, axis=-1, keepdims=True) / width
    total = jnp.zeros((rows_ref.shape[0], lanes), jnp.float32)
    for c in range(width // lanes):
        shifted = rows_ref[:, c * lanes : (c + 1) * lanes].astype(jnp.float32) - mean
        total = total + shifted * shifted
    spread = jnp.sum(total, axis=-1, keepdims=True) / width
    inverse = 1.0 / jnp.sqrt(spread + 1e-06)
    for j in range(count):
        start = pl.multiple_of(order[j] * depth, 128)
        part = rows_ref[:, pl.ds(start, depth)].astype(jnp.float32)
        out_ref[:, j * depth : (j + 1) * depth] = ((part - mean) * inverse).astype(jnp.bfloat16)


def ordered_norm(video_rows, order):
    rows, width = video_rows.shape
    tile = min(rows, 128)
    depth = width // order.shape[0]
    if depth % 128:
        normed = ordered_norm(video_rows, jnp.zeros((1,), jnp.int32))
        return jnp.concatenate(
            [take(normed, order[j], depth, 1) for j in range(order.shape[0])], axis=1
        )
    return pl.pallas_call(
        norm_kernel,
        grid_spec=pltpu.PrefetchScalarGridSpec(
            num_scalar_prefetch=1,
            grid=(rows // tile,),
            in_specs=[pl.BlockSpec((tile, width), lambda i, order: (i, 0))],
            out_specs=pl.BlockSpec((tile, width), lambda i, order: (i, 0)),
        ),
        out_shape=jax.ShapeDtypeStruct((rows, width), jnp.bfloat16),
        cost_estimate=pl.CostEstimate(
            flops=20 * rows * width, bytes_accessed=4 * rows * width, transcendentals=0
        ),
        name="ordered_norm",
    )(order, video_rows)


def attend_kernel(
    total_att, valid, queries_ref, square_ref, gain_ref, text_ref, places_ref, out_ref
):
    att = queries_ref.shape[1]
    root = jnp.sqrt(square_ref[...] / total_att + 1e-06)
    queries = (queries_ref[...] * (1.0 / root) * gain_ref[...]).astype(jnp.bfloat16)
    real = places_ref[...] < valid[0]
    for h in range(att // HD):
        own = slice(h * HD, (h + 1) * HD)
        keys = text_ref[:, own]
        values = text_ref[:, att + h * HD : att + (h + 1) * HD]
        scores = lax.dot_general(
            queries[:, own], keys, (((1,), (1,)), ((), ())), preferred_element_type=jnp.float32
        ) * HD ** (-0.5)
        scores = jnp.where(real, scores, jnp.float32(-1e30))
        shifted = jnp.exp(scores - jnp.max(scores, axis=-1, keepdims=True))
        inverse = 1.0 / jnp.sum(shifted, axis=-1, keepdims=True)
        weights = (shifted * inverse).astype(jnp.bfloat16)
        out_ref[:, own] = jnp.dot(weights, values, preferred_element_type=jnp.float32).astype(
            jnp.bfloat16
        )


def attend(queries, square, query_gain, text, places, valid_length, total_att):
    rows, att = queries.shape
    texts = text.shape[0]
    tile = min(rows, 256)
    return pl.pallas_call(
        functools.partial(attend_kernel, total_att),
        grid_spec=pltpu.PrefetchScalarGridSpec(
            num_scalar_prefetch=1,
            grid=(rows // tile,),
            in_specs=[
                pl.BlockSpec((tile, att), lambda i, v: (i, 0)),
                pl.BlockSpec((tile, 1), lambda i, v: (i, 0)),
                pl.BlockSpec((1, att), lambda i, v: (0, 0)),
                pl.BlockSpec((texts, 2 * att), lambda i, v: (0, 0)),
                pl.BlockSpec((1, texts), lambda i, v: (0, 0)),
            ],
            out_specs=pl.BlockSpec((tile, att), lambda i, v: (i, 0)),
        ),
        out_shape=jax.ShapeDtypeStruct((rows, att), jnp.bfloat16),
        cost_estimate=pl.CostEstimate(
            flops=4 * rows * att * texts,
            bytes_accessed=6 * rows * att + 4 * texts * att,
            transcendentals=rows * texts * att // HD,
        ),
        name="attend",
    )(valid_length, queries, square, query_gain[None, :], text, places[None, :])


VMEM = pl.BlockSpec(memory_space=pltpu.VMEM)
HBM = pl.BlockSpec(memory_space=pltpu.HBM)
SMEM = pl.BlockSpec(memory_space=pltpu.SMEM)


def call(kernel, outs, *args, flops=0, limit=24, specs=None, scratch=()):
    moved = sum(a.size * a.dtype.itemsize for a in args)
    moved += sum(o.size * o.dtype.itemsize for o in outs)
    return pl.pallas_call(
        kernel,
        out_shape=outs,
        in_specs=specs or [VMEM] * len(args),
        out_specs=[VMEM] * len(outs),
        scratch_shapes=scratch,
        compiler_params=pltpu.CompilerParams(vmem_limit_bytes=int(limit * 2**20)),
        cost_estimate=pl.CostEstimate(flops=flops, bytes_accessed=moved, transcendentals=0),
    )(*args)


def shape(*dims, dtype=jnp.bfloat16):
    return jax.ShapeDtypeStruct(dims, dtype)


def pack_kernel(context_ref, weight_ref, *refs):
    lay = Layout()
    out_refs, sems = refs[:-1], refs[-1]
    piece = weight_ref.shape[0] // lay.groups
    depth = context_ref.shape[1] // lay.seq
    copies = []

    def move(source, target):
        copies.append(pltpu.make_async_copy(source, target, sems.at[len(copies)]))
        copies[-1].start()

    for k, out_ref in enumerate(out_refs):
        group = lay.group ^ k
        for m in range(lay.mates):
            start = pl.multiple_of((group * lay.mates + (lay.mate ^ m)) * depth, 128)
            move(
                context_ref.at[:, pl.ds(start, depth)],
                out_ref.at[:, m * depth : (m + 1) * depth],
            )
        start = pl.multiple_of(group * piece, 16)
        move(weight_ref.at[pl.ds(start, piece), :], out_ref.at[:, lay.mates * depth :])
    for copy in copies:
        copy.wait()


def rows_norm_kernel(source_ref, out_ref, rows_ref, sems):
    lay = Layout()
    rows, width = rows_ref.shape
    parts = sems.shape[0]
    many = rows // parts
    copies = [
        pltpu.make_async_copy(
            source_ref.at[n * many : (n + 1) * many],
            rows_ref.at[n * many : (n + 1) * many],
            sems.at[n],
        )
        for n in range(parts)
    ]
    for copy in copies:
        copy.start()
    depth = width // lay.seq
    lanes, tile = 128, 32
    starts = [
        pl.multiple_of(
            ((lay.group ^ lay.mask(j, lay.mate ^ m)) * lay.mates + (lay.mate ^ m)) * depth, 128
        )
        for m in range(lay.mates)
        for j in range(lay.groups)
    ]

    def norm_tile(i):
        here = pl.ds(pl.multiple_of(i * tile, tile), tile)

        def part(c):
            return rows_ref[here, c * lanes : (c + 1) * lanes].astype(jnp.float32)

        sums = [jnp.zeros((tile, lanes), jnp.float32) for _ in range(4)]
        for c in range(width // lanes):
            sums[c % 4] = sums[c % 4] + part(c)
        mean = jnp.sum(sum(sums[1:], sums[0]), axis=-1, keepdims=True) / width
        mean = jnp.broadcast_to(mean, (tile, lanes))
        sums = [jnp.zeros((tile, lanes), jnp.float32) for _ in range(4)]
        for c in range(width // lanes):
            shifted = part(c) - mean
            sums[c % 4] = sums[c % 4] + shifted * shifted
        spread = jnp.sum(sum(sums[1:], sums[0]), axis=-1, keepdims=True) / width
        inverse = jnp.broadcast_to(1.0 / jnp.sqrt(spread + 1e-06), (tile, lanes))
        for j, start in enumerate(starts):
            for c in range(depth // lanes):
                source = pl.ds(pl.multiple_of(start + c * lanes, lanes), lanes)
                target = slice(j * depth + c * lanes, j * depth + (c + 1) * lanes)
                values = rows_ref[here, source].astype(jnp.float32)
                out_ref[here, target] = ((values - mean) * inverse).astype(jnp.bfloat16)

    for n, copy in enumerate(copies):
        copy.wait()
        pl.loop(n * many // tile, (n + 1) * many // tile)(norm_tile)


def text_kernel(depth, *refs):
    lay = Layout()
    got, refs = refs[: lay.groups], refs[lay.groups :]
    keys, refs = refs[: lay.mates], refs[lay.mates :]
    values, refs = refs[: lay.mates], refs[lay.mates :]
    totals, pieces_ref = refs[: lay.groups], refs[lay.groups]
    att = keys[0].shape[1]
    local = got[0].shape[0]
    rows = [
        jnp.concatenate([g[:, m * depth : (m + 1) * depth] for g in got], axis=0)
        for m in range(lay.mates)
    ]
    for at, weights in ((0, keys), (att, values)):
        total = dot32(rows[0], weights[0][...])
        for m in range(1, lay.mates):
            total = total + dot32(rows[m], weights[m][...])
        for k in range(lay.groups):
            totals[k][:, at : at + att] = total[k * local : (k + 1) * local]
    for k in range(lay.groups):
        spot = lay.group ^ lay.plane ^ k
        pieces_ref[pl.ds(spot, 1)] = got[k][:, lay.mates * depth :][None]


def to_row(column):
    return jnp.transpose(jnp.broadcast_to(column, (column.shape[0], 128)))[:1]


def to_column(row):
    wide = jnp.broadcast_to(row, (128, row.shape[1]))
    return jnp.transpose(wide)[:, :1]


def queries_kernel(*refs):
    normed_ref, weights, (out_ref, square_ref) = refs[0], refs[1:-2], refs[-2:]
    rows = normed_ref.shape[0]
    tile = min(rows, 256)
    for t in range(rows // tile):
        here = slice(t * tile, (t + 1) * tile)
        total, at = None, 0
        for weight_ref in weights:
            depth = weight_ref.shape[0]
            term = dot32(normed_ref[here, at : at + depth], weight_ref[...])
            total = term if total is None else total + term
            at += depth
        out_ref[here] = total
        square_ref[:, here] = to_row(jnp.sum(total * total, axis=1, keepdims=True))


def head_kernel(head, total_att, local, valid_ref, queries_ref, square_ref, gain_ref, *refs):
    lay = Layout()
    texts, out_ref = refs[:-1], refs[-1]
    rows, att = queries_ref.shape
    count = texts[0].shape[0]
    column = lax.broadcasted_iota(jnp.int32, (1, count), 1)
    reals = []
    for m in range(lay.mates):
        place = column % local
        for k in range(lay.groups):
            base = ((lay.group ^ k) * lay.mates + (lay.mate ^ m)) * local
            place = place + jnp.where(column // local == k, base, 0)
        reals.append(place < valid_ref[0])
    real = jnp.concatenate(reals, axis=1)
    tile = min(rows, 128)
    own = slice(head * HD, (head + 1) * HD)
    keys = jnp.concatenate([t[:, own] for t in texts], axis=0)
    at = slice(att + head * HD, att + (head + 1) * HD)
    values = jnp.concatenate([t[:, at] for t in texts], axis=0)
    for i in range(rows // tile):
        here = slice(i * tile, (i + 1) * tile)
        root = jnp.sqrt(to_column(square_ref[:, here]) / total_att + 1e-06)
        query = (queries_ref[here, own] * (1.0 / root) * gain_ref[:, own]).astype(jnp.bfloat16)
        scores = lax.dot_general(
            query, keys, (((1,), (1,)), ((), ())), preferred_element_type=jnp.float32
        ) * HD ** (-0.5)
        scores = jnp.where(real, scores, jnp.float32(-1e30))
        shifted = jnp.exp(scores - jnp.max(scores, axis=-1, keepdims=True))
        inverse = 1.0 / jnp.sum(shifted, axis=-1, keepdims=True)
        weights = (shifted * inverse).astype(jnp.bfloat16)
        out_ref[here] = dot32(weights, values).astype(jnp.bfloat16)


def place_kernel(*refs):
    lay = Layout()
    pieces, out_ref = refs[:-1], refs[-1]
    piece, cols = pieces[0].shape[2:]
    each = len(pieces) // lay.mates
    for m in range(lay.mates):
        at = pl.multiple_of((lay.mate ^ m) * cols, 128)
        j = 0
        for ref in pieces[m * each : (m + 1) * each]:
            for n in range(ref.shape[0]):
                row = pl.multiple_of((lay.group ^ lay.mask(j, lay.mate ^ m)) * piece, 16)
                out_ref[:, pl.ds(row, piece), pl.ds(at, cols)] = ref[n]
                j += 1


def side_by_side(pieces, here):
    return jnp.concatenate([p[here] for p in pieces], axis=1)


def most_kernel(count, heads, *refs):
    lay = Layout()
    weight_ref, video_ref, out_ref, part_ref, sem = refs[-5:]
    rows, width = out_ref.shape
    start = pl.multiple_of(lay.plane * width, 128)
    copy = pltpu.make_async_copy(video_ref.at[:, pl.ds(start, width)], part_ref, sem)
    copy.start()
    tile = min(rows, 128)
    for i in range(rows // tile):
        here = slice(i * tile, (i + 1) * tile)
        total = None
        for n in range(count):
            left = side_by_side(refs[n * heads : (n + 1) * heads], here)
            term = dot32(left, weight_ref[n])
            total = term if total is None else total + term
        if i == 0:
            copy.wait()
        out_ref[here] = total + part_ref[here].astype(jnp.float32)


def last_kernel(last, heads, *refs):
    pieces, (partial_ref, weight_ref, out_ref, copy_ref, sums_ref) = refs[:heads], refs[heads:]
    rows = out_ref.shape[0]
    tile = min(rows, 128)
    for i in range(rows // tile):
        here = slice(i * tile, (i + 1) * tile)
        total = partial_ref[here] + dot32(side_by_side(pieces, here), weight_ref[last])
        resid = total.astype(jnp.bfloat16)
        out_ref[here] = resid
        copy_ref[here] = resid
        resid = resid.astype(jnp.float32)
        sums_ref[0:1, here] = to_row(jnp.sum(resid, axis=1, keepdims=True))
        sums_ref[1:2, here] = to_row(jnp.sum(resid * resid, axis=1, keepdims=True))


def modulate_kernel(full_width, resid_ref, sums_ref, shift_ref, scale_ref, out_ref):
    rows = out_ref.shape[0]
    tile = min(rows, 128)
    for i in range(rows // tile):
        here = slice(i * tile, (i + 1) * tile)
        mean = to_column(sums_ref[0:1, here]) / full_width
        square = to_column(sums_ref[1:2, here]) / full_width
        inverse = 1.0 / jnp.sqrt(square - mean * mean + 1e-06)
        resid = resid_ref[here].astype(jnp.float32)
        out_ref[here] = (
            (resid - mean) * inverse * (1.0 + scale_ref[...]) + shift_ref[...]
        ).astype(jnp.bfloat16)


def aligned_path(
    lay,
    video_rows,
    context,
    valid_length,
    timestep,
    query_weight,
    key_weight,
    value_weight,
    out_weight,
    query_gain,
    key_gain,
    time_weight,
    modulation,
):
    f32 = jnp.float32
    rows, width = video_rows.shape
    local = context.shape[0]
    depth, att = key_weight.shape
    piece, cols = out_weight.shape[0] // lay.groups, out_weight.shape[1]
    width_local = modulation.shape[1]
    total_att = att * lay.head

    packed = lay.mates * depth + cols
    sent = call(
        pack_kernel,
        [shape(local, packed)] * lay.groups,
        context,
        out_weight,
        specs=[HBM] * 2,
        limit=62.65,
        scratch=[pltpu.SemaphoreType.DMA((lay.groups * (lay.mates + 1),))],
    )
    got = [lay.to_peer(x, k) for k, x in enumerate(sent)]
    key_parts = [lay.to_mate(key_weight, m) for m in range(lay.mates)]
    value_parts = [lay.to_mate(value_weight, m) for m in range(lay.mates)]
    (normed,) = call(
        rows_norm_kernel,
        [shape(rows, width)],
        video_rows,
        flops=40 * rows * width,
        specs=[HBM],
        scratch=[pltpu.VMEM((rows, width), jnp.bfloat16), pltpu.SemaphoreType.DMA((4,))],
    )
    mine = lay.double(query_weight)
    *totals, pieces = call(
        functools.partial(text_kernel, depth),
        [shape(local, 2 * att, dtype=f32)] * lay.groups + [shape(lay.head, piece, cols)],
        *got,
        *key_parts,
        *value_parts,
        flops=4 * local * lay.groups * lay.mates * depth * att,
    )
    total = totals[0]
    for k in range(1, lay.groups):
        total = total + lay.to_peer(totals[k], k)
    keys, values = total[:, :att], total[:, att:]
    square = lay.plane_sum(jnp.sum(keys * keys, axis=1))
    keys = (keys / jnp.sqrt(square[:, None] / total_att + 1e-06) * key_gain).astype(
        jnp.bfloat16
    )
    text = jnp.concatenate([keys, values.astype(jnp.bfloat16)], axis=1)
    text = jnp.concatenate([lay.to_peer(text, k) for k in range(lay.groups)], axis=0)
    texts = [lay.to_mate(text, m) for m in range(lay.mates)]

    queries, square = call(
        queries_kernel,
        [shape(rows, att, dtype=f32), shape(1, rows, dtype=f32)],
        normed,
        *[x for m in range(lay.mates) for x in lay.to_mate_each(mine, m)],
        flops=2 * rows * width * att,
    )
    square = lay.plane_sum(square)

    held = {d: [pieces[d]] for d in range(lay.head)}
    crossed, spots = cross_held(lay, held)
    mine = lay.double(crossed[None])
    (weights,) = call(
        place_kernel,
        [shape(lay.head, out_weight.shape[0], width_local)],
        *[x for m in range(lay.mates) for x in lay.to_mate_each(mine, m)],
        flops=width_local * width,
    )

    heads = att // HD
    spread = []
    for h in range(heads):
        (attended,) = call(
            functools.partial(head_kernel, h, total_att, local),
            [shape(rows, HD)],
            valid_length,
            queries,
            square,
            query_gain[None, :],
            *texts,
            flops=8 * rows * HD * local * lay.seq,
            specs=[SMEM] + [VMEM] * (3 + lay.mates),
        )
        spread.append(spread_planes(lay, attended))
    most = lay.head - 1
    (partial,) = call(
        functools.partial(most_kernel, most, heads),
        [shape(rows, width_local, dtype=f32)],
        *[spread[h][d] for d in spots[:-1] for h in range(heads)],
        weights,
        video_rows,
        flops=2 * most * rows * att * width_local,
        specs=[VMEM] * (most * heads + 1) + [HBM],
        scratch=[pltpu.VMEM((rows, width_local), jnp.bfloat16), pltpu.SemaphoreType.DMA],
    )
    residual_out, resid, sums = call(
        functools.partial(last_kernel, most, heads),
        [shape(rows, width_local)] * 2 + [shape(2, rows, dtype=f32)],
        *[spread[h][spots[-1]] for h in range(heads)],
        partial,
        weights,
        flops=2 * rows * att * width_local,
    )
    sums = lay.plane_sum(sums)
    shift, scale = shift_and_scale(timestep, time_weight, modulation)
    (modulated,) = call(
        functools.partial(modulate_kernel, width_local * lay.head),
        [shape(rows, width_local)],
        resid,
        sums,
        shift[None, :],
        scale[None, :],
        flops=8 * rows * width_local,
    )
    return residual_out, modulated


def first_exchange(lay, context, out_weight, depth):
    piece = out_weight.shape[0] // lay.groups
    text_local = context.shape[0]
    texts, pieces = [], []
    for k in range(lay.groups):
        columns = [
            take(context, (lay.group ^ k) * lay.mates + (lay.mate ^ m), depth, 1)
            for m in range(lay.mates)
        ]
        rows = take(out_weight, lay.group ^ k, piece, 0).reshape(text_local, -1)
        both = lay.to_peer(jnp.concatenate(columns + [rows], axis=1), k)
        texts.append(both[:, : lay.mates * depth])
        pieces.append(both[:, lay.mates * depth :].reshape(piece, -1))
    return jnp.concatenate(texts, axis=0), jnp.stack(pieces)


def cross_planes(lay, pieces):
    held = {d: [pick(pieces, lay.group ^ lay.plane ^ d)] for d in range(lay.head)}
    return cross_held(lay, held)


def cross_held(lay, held):
    spots = [0]
    step = lay.head // 2
    while step:
        sent = jnp.stack([x for d in range(step) for x in held[d + step]])
        got = lay.to_plane(sent, step)
        many = len(held[0])
        for d in range(step):
            held[d] = held[d] + [got[d * many + n] for n in range(many)]
        spots = spots + [s ^ step for s in spots]
        step //= 2
    return jnp.stack(held[0]), spots


def gather_out_weight(lay, pieces):
    crossed, spots = cross_planes(lay, pieces)
    mine = jnp.concatenate(lay.double(crossed[None]), axis=0)
    both = jnp.stack([lay.to_mate(mine, m) for m in range(lay.mates)])
    columns = []
    for m in range(lay.mates):
        half = pick(both, lay.mate ^ m)
        slots = []
        for g in range(lay.groups):
            distance = lay.group ^ g
            slot = sum(
                jnp.where(lay.mask(j, jnp.int32(m)) == distance, j, 0)
                for j in range(lay.groups)
            )
            slots.append(pick(half, slot))
        columns.append(jnp.concatenate(slots, axis=1))
    return jnp.concatenate(columns, axis=2), spots


def project_text(lay, texts, key_weight, value_weight, key_gain, total_att):
    att = key_weight.shape[1]
    pair = jnp.concatenate([key_weight, value_weight], axis=1)
    weights = jnp.concatenate([lay.to_mate(pair, m) for m in range(lay.mates)], axis=0)
    partial = dot32(texts, weights)
    local = texts.shape[0] // lay.groups
    total = partial[:local]
    for k in range(1, lay.groups):
        total = total + lay.to_peer(partial[k * local : (k + 1) * local], k)
    keys, values = total[:, :att], total[:, att:]
    square = lay.plane_sum(jnp.sum(keys * keys, axis=1))
    keys = (keys / jnp.sqrt(square[:, None] / total_att + 1e-06) * key_gain).astype(
        jnp.bfloat16
    )
    packed = jnp.concatenate([keys, values.astype(jnp.bfloat16)], axis=1)
    packed = jnp.concatenate([lay.to_peer(packed, k) for k in range(lay.groups)], axis=0)
    packed = jnp.concatenate([lay.to_mate(packed, m) for m in range(lay.mates)], axis=0)
    places = jnp.concatenate(
        [
            ((lay.group ^ k) * lay.mates + (lay.mate ^ m)) * local
            + jnp.arange(local, dtype=jnp.int32)
            for m in range(lay.mates)
            for k in range(lay.groups)
        ]
    )
    return packed, places


def project_queries(lay, video_rows, query_weight):
    order = jnp.stack(
        [
            (lay.group ^ lay.mask(j, lay.mate ^ m)) * lay.mates + (lay.mate ^ m)
            for m in range(lay.mates)
            for j in range(lay.groups)
        ]
    ).astype(jnp.int32)
    normed = ordered_norm(video_rows, order)
    mine = jnp.concatenate(lay.double(query_weight), axis=0)
    depth = mine.shape[0]
    queries = None
    for m in range(lay.mates):
        term = dot32(normed[:, m * depth : (m + 1) * depth], lay.to_mate(mine, m))
        queries = term if queries is None else queries + term
    return queries, lay.plane_sum(jnp.sum(queries * queries, axis=1))


def spread_planes(lay, attended):
    have = {0: attended}
    step = lay.head // 2
    while step:
        for d in sorted(have):
            have[d ^ step] = lay.to_plane(have[d], step)
        step //= 2
    return have


def shift_and_scale(timestep, time_weight, modulation):
    half = FREQ // 2
    freqs = jnp.exp(-jnp.log(10000.0) * jnp.arange(half, dtype=jnp.float32) / half)
    angles = timestep[0].astype(jnp.float32) * freqs
    embedding = jnp.concatenate([jnp.cos(angles), jnp.sin(angles)])
    act = jax.nn.silu(embedding).astype(jnp.bfloat16)[None, :]
    shift = modulation[0] + dot32(act, time_weight[0])[0]
    scale = modulation[1] + dot32(act, time_weight[1])[0]
    return shift, scale


def on_device(
    video_rows,
    context,
    valid_length,
    timestep,
    query_weight,
    key_weight,
    value_weight,
    out_weight,
    query_gain,
    key_gain,
    time_weight,
    modulation,
):
    lay = Layout()
    if query_weight.shape[0] % 128 == 0 and out_weight.shape[0] == lay.groups * context.shape[0]:
        return aligned_path(
            lay,
            video_rows,
            context,
            valid_length,
            timestep,
            query_weight,
            key_weight,
            value_weight,
            out_weight,
            query_gain,
            key_gain,
            time_weight,
            modulation,
        )
    total_att = query_weight.shape[1] * lay.head
    width_local = modulation.shape[1]
    texts, pieces = first_exchange(lay, context, out_weight, key_weight.shape[0])
    text, places = project_text(lay, texts, key_weight, value_weight, key_gain, total_att)
    queries, square = project_queries(lay, video_rows, query_weight)
    block_rows, spots = gather_out_weight(lay, pieces)
    attended = attend(
        queries, square[:, None], query_gain, text, places, valid_length, total_att
    )
    spread = spread_planes(lay, attended)
    projected = None
    for n, d in enumerate(spots):
        term = dot32(spread[d], block_rows[n])
        projected = term if projected is None else projected + term
    video_part = take(video_rows, lay.plane, width_local, 1)
    residual_out = (video_part.astype(jnp.float32) + projected).astype(jnp.bfloat16)
    shift, scale = shift_and_scale(timestep, time_weight, modulation)
    resid = residual_out.astype(jnp.float32)
    sums = lay.plane_sum(jnp.stack([jnp.sum(resid, axis=1), jnp.sum(resid * resid, axis=1)]))
    full_width = width_local * lay.head
    mean2 = (sums[0] / full_width)[:, None]
    var2 = (sums[1] / full_width)[:, None] - mean2 * mean2
    modulated = ((resid - mean2) / jnp.sqrt(var2 + 1e-06) * (1.0 + scale) + shift).astype(
        jnp.bfloat16
    )
    return (residual_out, modulated)


def solution(mesh):
    in_specs = (
        P("seq", None),
        P("seq", None),
        P(),
        P(),
        P("seq", "head"),
        P("seq", "head"),
        P("seq", "head"),
        P("head", "seq"),
        P("head"),
        P("head"),
        P(None, None, "head"),
        P(None, "head"),
    )
    out_specs = (P("seq", "head"), P("seq", "head"))
    return jax.shard_map(
        on_device, mesh=mesh, in_specs=in_specs, out_specs=out_specs, check_vma=False
    )
```

```python
import functools

import jax
import jax.numpy as jnp
from jax import lax
from jax.experimental import pallas as pl
from jax.experimental.pallas import tpu as pltpu
from jax.sharding import PartitionSpec as P


HD = 128
FREQ = 256


def dot32(left, right):
    return jnp.dot(left, right, preferred_element_type=jnp.float32)


def take(x, index, size, axis):
    return lax.dynamic_slice_in_dim(x, index * size, size, axis)


def pick(x, index):
    return lax.dynamic_index_in_dim(x, index, 0, False)


class Layout:
    def __init__(self):
        self.seq = lax.axis_size("seq")
        self.head = lax.axis_size("head")
        self.mates = self.seq // self.head
        self.groups = self.seq // self.mates
        self.bits = self.groups.bit_length() - 1
        index = lax.axis_index("seq")
        self.group = index // self.mates
        self.mate = index % self.mates
        self.plane = lax.axis_index("head")

    def permute(self, x, axis, pairs):
        return lax.ppermute(x, axis, pairs)

    def to_peer(self, x, k):
        if k == 0:
            return x
        pairs = [
            (g * self.mates + m, (g ^ k) * self.mates + m)
            for g in range(self.groups)
            for m in range(self.mates)
        ]
        return self.permute(x, "seq", pairs)

    def to_mate(self, x, m):
        if m == 0:
            return x
        return self.permute(x, "seq", [(i, i ^ m) for i in range(self.seq)])

    def to_plane(self, x, k):
        if k == 0:
            return x
        return self.permute(x, "head", [(i, i ^ k) for i in range(self.head)])

    def turned(self, step, m):
        return 1 << ((step + m) % self.bits)

    def double(self, x):
        have = [x]
        for step in range(self.bits):
            pairs = [
                (g * self.mates + m, (g ^ self.turned(step, m)) * self.mates + m)
                for g in range(self.groups)
                for m in range(self.mates)
            ]
            whole = jnp.concatenate(have, axis=0) if step else x
            have.append(self.permute(whole, "seq", pairs))
        return have

    def to_mate_each(self, pieces, m):
        return [self.to_mate(x, m) for x in pieces]

    def mask(self, slot, mate):
        total = jnp.int32(0)
        for m in range(self.mates):
            value = 0
            for step in range(self.bits):
                if slot >> step & 1:
                    value |= self.turned(step, m)
            total = total + jnp.where(mate == m, value, 0)
        return total

    def plane_sum(self, x):
        total = x
        for k in range(1, self.head):
            total = total + self.to_plane(x, k)
        return total


def norm_kernel(order, rows_ref, out_ref):
    width = rows_ref.shape[1]
    count = order.shape[0]
    depth = width // count
    lanes = 128
    total = jnp.zeros((rows_ref.shape[0], lanes), jnp.float32)
    for c in range(width // lanes):
        total = total + rows_ref[:, c * lanes : (c + 1) * lanes].astype(jnp.float32)
    mean = jnp.sum(total, axis=-1, keepdims=True) / width
    total = jnp.zeros((rows_ref.shape[0], lanes), jnp.float32)
    for c in range(width // lanes):
        shifted = rows_ref[:, c * lanes : (c + 1) * lanes].astype(jnp.float32) - mean
        total = total + shifted * shifted
    spread = jnp.sum(total, axis=-1, keepdims=True) / width
    inverse = 1.0 / jnp.sqrt(spread + 1e-06)
    for j in range(count):
        start = pl.multiple_of(order[j] * depth, 128)
        part = rows_ref[:, pl.ds(start, depth)].astype(jnp.float32)
        out_ref[:, j * depth : (j + 1) * depth] = ((part - mean) * inverse).astype(jnp.bfloat16)


def ordered_norm(video_rows, order):
    rows, width = video_rows.shape
    tile = min(rows, 128)
    depth = width // order.shape[0]
    if depth % 128:
        normed = ordered_norm(video_rows, jnp.zeros((1,), jnp.int32))
        return jnp.concatenate(
            [take(normed, order[j], depth, 1) for j in range(order.shape[0])], axis=1
        )
    return pl.pallas_call(
        norm_kernel,
        grid_spec=pltpu.PrefetchScalarGridSpec(
            num_scalar_prefetch=1,
            grid=(rows // tile,),
            in_specs=[pl.BlockSpec((tile, width), lambda i, order: (i, 0))],
            out_specs=pl.BlockSpec((tile, width), lambda i, order: (i, 0)),
        ),
        out_shape=jax.ShapeDtypeStruct((rows, width), jnp.bfloat16),
        cost_estimate=pl.CostEstimate(
            flops=20 * rows * width, bytes_accessed=4 * rows * width, transcendentals=0
        ),
        name="ordered_norm",
    )(order, video_rows)


def attend_kernel(
    total_att, valid, queries_ref, square_ref, gain_ref, text_ref, places_ref, out_ref
):
    att = queries_ref.shape[1]
    root = jnp.sqrt(square_ref[...] / total_att + 1e-06)
    queries = (queries_ref[...] * (1.0 / root) * gain_ref[...]).astype(jnp.bfloat16)
    real = places_ref[...] < valid[0]
    for h in range(att // HD):
        own = slice(h * HD, (h + 1) * HD)
        keys = text_ref[:, own]
        values = text_ref[:, att + h * HD : att + (h + 1) * HD]
        scores = lax.dot_general(
            queries[:, own], keys, (((1,), (1,)), ((), ())), preferred_element_type=jnp.float32
        ) * HD ** (-0.5)
        scores = jnp.where(real, scores, jnp.float32(-1e30))
        shifted = jnp.exp(scores - jnp.max(scores, axis=-1, keepdims=True))
        inverse = 1.0 / jnp.sum(shifted, axis=-1, keepdims=True)
        weights = (shifted * inverse).astype(jnp.bfloat16)
        out_ref[:, own] = jnp.dot(weights, values, preferred_element_type=jnp.float32).astype(
            jnp.bfloat16
        )


def attend(queries, square, query_gain, text, places, valid_length, total_att):
    rows, att = queries.shape
    texts = text.shape[0]
    tile = min(rows, 256)
    return pl.pallas_call(
        functools.partial(attend_kernel, total_att),
        grid_spec=pltpu.PrefetchScalarGridSpec(
            num_scalar_prefetch=1,
            grid=(rows // tile,),
            in_specs=[
                pl.BlockSpec((tile, att), lambda i, v: (i, 0)),
                pl.BlockSpec((tile, 1), lambda i, v: (i, 0)),
                pl.BlockSpec((1, att), lambda i, v: (0, 0)),
                pl.BlockSpec((texts, 2 * att), lambda i, v: (0, 0)),
                pl.BlockSpec((1, texts), lambda i, v: (0, 0)),
            ],
            out_specs=pl.BlockSpec((tile, att), lambda i, v: (i, 0)),
        ),
        out_shape=jax.ShapeDtypeStruct((rows, att), jnp.bfloat16),
        cost_estimate=pl.CostEstimate(
            flops=4 * rows * att * texts,
            bytes_accessed=6 * rows * att + 4 * texts * att,
            transcendentals=rows * texts * att // HD,
        ),
        name="attend",
    )(valid_length, queries, square, query_gain[None, :], text, places[None, :])


VMEM = pl.BlockSpec(memory_space=pltpu.VMEM)
HBM = pl.BlockSpec(memory_space=pltpu.HBM)
SMEM = pl.BlockSpec(memory_space=pltpu.SMEM)


def call(kernel, outs, *args, flops=0, limit=24, specs=None, outs_at=None, scratch=()):
    moved = sum(a.size * a.dtype.itemsize for a in args)
    moved += sum(o.size * o.dtype.itemsize for o in outs)
    return pl.pallas_call(
        kernel,
        out_shape=outs,
        in_specs=specs or [VMEM] * len(args),
        out_specs=outs_at or [VMEM] * len(outs),
        scratch_shapes=scratch,
        compiler_params=pltpu.CompilerParams(vmem_limit_bytes=int(limit * 2**20)),
        cost_estimate=pl.CostEstimate(flops=flops, bytes_accessed=moved, transcendentals=0),
    )(*args)


def shape(*dims, dtype=jnp.bfloat16):
    return jax.ShapeDtypeStruct(dims, dtype)


def pack_kernel(context_hbm, weight_hbm, *refs):
    lay = Layout()
    out_refs, (context_ref, weight_ref, sems) = refs[: lay.groups], refs[lay.groups :]
    copies = [
        pltpu.make_async_copy(context_hbm, context_ref, sems.at[0]),
        pltpu.make_async_copy(weight_hbm, weight_ref, sems.at[1]),
    ]
    for copy in copies:
        copy.start()
    for copy in copies:
        copy.wait()
    piece = weight_ref.shape[0] // lay.groups
    depth = context_ref.shape[1] // lay.seq
    for k, out_ref in enumerate(out_refs):
        group = lay.group ^ k
        for m in range(lay.mates):
            start = pl.multiple_of((group * lay.mates + (lay.mate ^ m)) * depth, 128)
            out_ref[:, m * depth : (m + 1) * depth] = context_ref[:, pl.ds(start, depth)]
        start = pl.multiple_of(group * piece, 16)
        out_ref[:, lay.mates * depth :] = weight_ref[pl.ds(start, piece), :]


def rows_norm_kernel(source_ref, out_ref, rows_ref, sems):
    lay = Layout()
    rows, width = rows_ref.shape
    parts = sems.shape[0]
    many = rows // parts
    copies = [
        pltpu.make_async_copy(
            source_ref.at[n * many : (n + 1) * many],
            rows_ref.at[n * many : (n + 1) * many],
            sems.at[n],
        )
        for n in range(parts)
    ]
    for copy in copies:
        copy.start()
    depth = width // lay.seq
    lanes, tile = 128, 32
    starts = [
        pl.multiple_of(
            ((lay.group ^ lay.mask(j, lay.mate ^ m)) * lay.mates + (lay.mate ^ m)) * depth, 128
        )
        for m in range(lay.mates)
        for j in range(lay.groups)
    ]

    def norm_tile(i):
        here = pl.ds(pl.multiple_of(i * tile, tile), tile)

        def part(c):
            return rows_ref[here, c * lanes : (c + 1) * lanes].astype(jnp.float32)

        sums = [jnp.zeros((tile, lanes), jnp.float32) for _ in range(4)]
        for c in range(width // lanes):
            sums[c % 4] = sums[c % 4] + part(c)
        mean = jnp.sum(sum(sums[1:], sums[0]), axis=-1, keepdims=True) / width
        mean = jnp.broadcast_to(mean, (tile, lanes))
        sums = [jnp.zeros((tile, lanes), jnp.float32) for _ in range(4)]
        for c in range(width // lanes):
            shifted = part(c) - mean
            sums[c % 4] = sums[c % 4] + shifted * shifted
        spread = jnp.sum(sum(sums[1:], sums[0]), axis=-1, keepdims=True) / width
        inverse = jnp.broadcast_to(1.0 / jnp.sqrt(spread + 1e-06), (tile, lanes))
        for j, start in enumerate(starts):
            for c in range(depth // lanes):
                source = pl.ds(pl.multiple_of(start + c * lanes, lanes), lanes)
                target = slice(j * depth + c * lanes, j * depth + (c + 1) * lanes)
                values = rows_ref[here, source].astype(jnp.float32)
                out_ref[here, target] = ((values - mean) * inverse).astype(jnp.bfloat16)

    for n, copy in enumerate(copies):
        copy.wait()
        pl.loop(n * many // tile, (n + 1) * many // tile)(norm_tile)


def text_kernel(depth, *refs):
    lay = Layout()
    got, refs = refs[: lay.groups], refs[lay.groups :]
    keys, refs = refs[: lay.mates], refs[lay.mates :]
    values, refs = refs[: lay.mates], refs[lay.mates :]
    totals, pieces_ref = refs[: lay.groups], refs[lay.groups]
    att = keys[0].shape[1]
    local = got[0].shape[0]
    rows = [
        jnp.concatenate([g[:, m * depth : (m + 1) * depth] for g in got], axis=0)
        for m in range(lay.mates)
    ]
    for at, weights in ((0, keys), (att, values)):
        total = dot32(rows[0], weights[0][...])
        for m in range(1, lay.mates):
            total = total + dot32(rows[m], weights[m][...])
        for k in range(lay.groups):
            totals[k][:, at : at + att] = total[k * local : (k + 1) * local]
    for k in range(lay.groups):
        spot = lay.group ^ lay.plane ^ k
        pieces_ref[pl.ds(spot, 1)] = got[k][:, lay.mates * depth :][None]


def to_row(column):
    return jnp.transpose(jnp.broadcast_to(column, (column.shape[0], 128)))[:1]


def to_column(row):
    wide = jnp.broadcast_to(row, (128, row.shape[1]))
    return jnp.transpose(wide)[:, :1]


def queries_kernel(*refs):
    normed_ref, weights, (out_ref, square_ref) = refs[0], refs[1:-2], refs[-2:]
    rows = normed_ref.shape[0]
    tile = min(rows, 256)
    for t in range(rows // tile):
        here = slice(t * tile, (t + 1) * tile)
        total, at = None, 0
        for weight_ref in weights:
            depth = weight_ref.shape[0]
            term = dot32(normed_ref[here, at : at + depth], weight_ref[...])
            total = term if total is None else total + term
            at += depth
        out_ref[here] = total
        square_ref[:, here] = to_row(jnp.sum(total * total, axis=1, keepdims=True))


def head_kernel(head, total_att, local, valid_ref, queries_ref, square_ref, gain_ref, *refs):
    lay = Layout()
    texts, out_ref = refs[:-1], refs[-1]
    rows, att = queries_ref.shape
    count = texts[0].shape[0]
    column = lax.broadcasted_iota(jnp.int32, (1, count), 1)
    reals = []
    for m in range(lay.mates):
        place = column % local
        for k in range(lay.groups):
            base = ((lay.group ^ k) * lay.mates + (lay.mate ^ m)) * local
            place = place + jnp.where(column // local == k, base, 0)
        reals.append(place < valid_ref[0])
    real = jnp.concatenate(reals, axis=1)
    tile = min(rows, 128)
    own = slice(head * HD, (head + 1) * HD)
    keys = jnp.concatenate([t[:, own] for t in texts], axis=0)
    at = slice(att + head * HD, att + (head + 1) * HD)
    values = jnp.concatenate([t[:, at] for t in texts], axis=0)
    for i in range(rows // tile):
        here = slice(i * tile, (i + 1) * tile)
        root = jnp.sqrt(to_column(square_ref[:, here]) / total_att + 1e-06)
        query = (queries_ref[here, own] * (1.0 / root) * gain_ref[:, own]).astype(jnp.bfloat16)
        scores = lax.dot_general(
            query, keys, (((1,), (1,)), ((), ())), preferred_element_type=jnp.float32
        ) * HD ** (-0.5)
        scores = jnp.where(real, scores, jnp.float32(-1e30))
        shifted = jnp.exp(scores - jnp.max(scores, axis=-1, keepdims=True))
        inverse = 1.0 / jnp.sum(shifted, axis=-1, keepdims=True)
        weights = (shifted * inverse).astype(jnp.bfloat16)
        out_ref[here] = dot32(weights, values).astype(jnp.bfloat16)


def place_kernel(*refs):
    lay = Layout()
    pieces, out_ref = refs[:-1], refs[-1]
    piece, cols = pieces[0].shape[2:]
    each = len(pieces) // lay.mates
    for m in range(lay.mates):
        at = pl.multiple_of((lay.mate ^ m) * cols, 128)
        j = 0
        for ref in pieces[m * each : (m + 1) * each]:
            for n in range(ref.shape[0]):
                row = pl.multiple_of((lay.group ^ lay.mask(j, lay.mate ^ m)) * piece, 16)
                out_ref[:, pl.ds(row, piece), pl.ds(at, cols)] = ref[n]
                j += 1


def side_by_side(pieces, here):
    return jnp.concatenate([p[here] for p in pieces], axis=1)


def most_kernel(count, heads, *refs):
    lay = Layout()
    weight_ref, video_ref, out_ref, part_ref, sem = refs[-5:]
    rows, width = out_ref.shape
    start = pl.multiple_of(lay.plane * width, 128)
    copy = pltpu.make_async_copy(video_ref.at[:, pl.ds(start, width)], part_ref, sem)
    copy.start()
    tile = min(rows, 128)
    for i in range(rows // tile):
        here = slice(i * tile, (i + 1) * tile)
        total = None
        for n in range(count):
            left = side_by_side(refs[n * heads : (n + 1) * heads], here)
            term = dot32(left, weight_ref[n])
            total = term if total is None else total + term
        if i == 0:
            copy.wait()
        out_ref[here] = total + part_ref[here].astype(jnp.float32)


def last_kernel(last, heads, *refs):
    pieces, (partial_ref, weight_ref, out_ref, sums_ref) = refs[:heads], refs[heads:]
    rows = out_ref.shape[0]
    tile = min(rows, 128)
    for i in range(rows // tile):
        here = slice(i * tile, (i + 1) * tile)
        total = partial_ref[here] + dot32(side_by_side(pieces, here), weight_ref[last])
        resid = total.astype(jnp.bfloat16)
        out_ref[here] = resid
        resid = resid.astype(jnp.float32)
        sums_ref[0:1, here] = to_row(jnp.sum(resid, axis=1, keepdims=True))
        sums_ref[1:2, here] = to_row(jnp.sum(resid * resid, axis=1, keepdims=True))


def modulate_kernel(
    full_width, resid_ref, sums_ref, shift_ref, scale_ref, first_ref, out_ref, tiles_ref, sems
):
    rows = resid_ref.shape[0]
    tile = min(rows, 128)
    copies = [pltpu.make_async_copy(resid_ref, first_ref, sems.at[0])]
    copies[0].start()
    for i in range(rows // tile):
        here = slice(i * tile, (i + 1) * tile)
        mean = to_column(sums_ref[0:1, here]) / full_width
        square = to_column(sums_ref[1:2, here]) / full_width
        inverse = 1.0 / jnp.sqrt(square - mean * mean + 1e-06)
        resid = resid_ref[here].astype(jnp.float32)
        tiles_ref[here] = (
            (resid - mean) * inverse * (1.0 + scale_ref[...]) + shift_ref[...]
        ).astype(jnp.bfloat16)
        copies.append(
            pltpu.make_async_copy(tiles_ref.at[here], out_ref.at[here], sems.at[i + 1])
        )
        copies[-1].start()
    for copy in copies:
        copy.wait()


def aligned_path(
    lay,
    video_rows,
    context,
    valid_length,
    timestep,
    query_weight,
    key_weight,
    value_weight,
    out_weight,
    query_gain,
    key_gain,
    time_weight,
    modulation,
):
    f32 = jnp.float32
    rows, width = video_rows.shape
    local = context.shape[0]
    depth, att = key_weight.shape
    piece, cols = out_weight.shape[0] // lay.groups, out_weight.shape[1]
    width_local = modulation.shape[1]
    total_att = att * lay.head

    packed = lay.mates * depth + cols
    sent = call(
        pack_kernel,
        [shape(local, packed)] * lay.groups,
        context,
        out_weight,
        specs=[HBM] * 2,
        limit=62.65,
        scratch=[
            pltpu.VMEM(context.shape, jnp.bfloat16),
            pltpu.VMEM(out_weight.shape, jnp.bfloat16),
            pltpu.SemaphoreType.DMA((2,)),
        ],
    )
    got = [lay.to_peer(x, k) for k, x in enumerate(sent)]
    key_parts = [lay.to_mate(key_weight, m) for m in range(lay.mates)]
    value_parts = [lay.to_mate(value_weight, m) for m in range(lay.mates)]
    (normed,) = call(
        rows_norm_kernel,
        [shape(rows, width)],
        video_rows,
        flops=40 * rows * width,
        specs=[HBM],
        scratch=[pltpu.VMEM((rows, width), jnp.bfloat16), pltpu.SemaphoreType.DMA((4,))],
    )
    mine = lay.double(query_weight)
    *totals, pieces = call(
        functools.partial(text_kernel, depth),
        [shape(local, 2 * att, dtype=f32)] * lay.groups + [shape(lay.head, piece, cols)],
        *got,
        *key_parts,
        *value_parts,
        flops=4 * local * lay.groups * lay.mates * depth * att,
    )
    total = totals[0]
    for k in range(1, lay.groups):
        total = total + lay.to_peer(totals[k], k)
    keys, values = total[:, :att], total[:, att:]
    queries, square = call(
        queries_kernel,
        [shape(rows, att, dtype=f32), shape(1, rows, dtype=f32)],
        normed,
        *[x for m in range(lay.mates) for x in lay.to_mate_each(mine, m)],
        flops=2 * rows * width * att,
    )
    square = jnp.concatenate([square, jnp.sum(keys * keys, axis=1)[None, :]], axis=1)
    square = lay.plane_sum(square)
    key_square, square = square[0, rows:, None], square[:, :rows]
    keys = (keys / jnp.sqrt(key_square / total_att + 1e-06) * key_gain).astype(jnp.bfloat16)
    text = jnp.concatenate([keys, values.astype(jnp.bfloat16)], axis=1)
    text = jnp.concatenate([lay.to_peer(text, k) for k in range(lay.groups)], axis=0)
    texts = [lay.to_mate(text, m) for m in range(lay.mates)]

    held = {d: [pieces[d]] for d in range(lay.head)}
    crossed, spots = cross_held(lay, held)
    mine = lay.double(crossed[None])
    (weights,) = call(
        place_kernel,
        [shape(lay.head, out_weight.shape[0], width_local)],
        *[x for m in range(lay.mates) for x in lay.to_mate_each(mine, m)],
        flops=width_local * width,
    )

    heads = att // HD
    spread = []
    for h in range(heads):
        (attended,) = call(
            functools.partial(head_kernel, h, total_att, local),
            [shape(rows, HD)],
            valid_length,
            queries,
            square,
            query_gain[None, :],
            *texts,
            flops=8 * rows * HD * local * lay.seq,
            specs=[SMEM] + [VMEM] * (3 + lay.mates),
        )
        spread.append(spread_planes(lay, attended))
    most = lay.head - 1
    (partial,) = call(
        functools.partial(most_kernel, most, heads),
        [shape(rows, width_local, dtype=f32)],
        *[spread[h][d] for d in spots[:-1] for h in range(heads)],
        weights,
        video_rows,
        flops=2 * most * rows * att * width_local,
        specs=[VMEM] * (most * heads + 1) + [HBM],
        scratch=[pltpu.VMEM((rows, width_local), jnp.bfloat16), pltpu.SemaphoreType.DMA],
    )
    resid, sums = call(
        functools.partial(last_kernel, most, heads),
        [shape(rows, width_local), shape(2, rows, dtype=f32)],
        *[spread[h][spots[-1]] for h in range(heads)],
        partial,
        weights,
        flops=2 * rows * att * width_local,
    )
    sums = lay.plane_sum(sums)
    shift, scale = shift_and_scale(timestep, time_weight, modulation)
    residual_out, modulated = call(
        functools.partial(modulate_kernel, width_local * lay.head),
        [shape(rows, width_local)] * 2,
        resid,
        sums,
        shift[None, :],
        scale[None, :],
        flops=8 * rows * width_local,
        outs_at=[HBM] * 2,
        scratch=[pltpu.VMEM((rows, width_local), jnp.bfloat16), pltpu.SemaphoreType.DMA((8,))],
    )
    return residual_out, modulated


def first_exchange(lay, context, out_weight, depth):
    piece = out_weight.shape[0] // lay.groups
    text_local = context.shape[0]
    texts, pieces = [], []
    for k in range(lay.groups):
        columns = [
            take(context, (lay.group ^ k) * lay.mates + (lay.mate ^ m), depth, 1)
            for m in range(lay.mates)
        ]
        rows = take(out_weight, lay.group ^ k, piece, 0).reshape(text_local, -1)
        both = lay.to_peer(jnp.concatenate(columns + [rows], axis=1), k)
        texts.append(both[:, : lay.mates * depth])
        pieces.append(both[:, lay.mates * depth :].reshape(piece, -1))
    return jnp.concatenate(texts, axis=0), jnp.stack(pieces)


def cross_planes(lay, pieces):
    held = {d: [pick(pieces, lay.group ^ lay.plane ^ d)] for d in range(lay.head)}
    return cross_held(lay, held)


def cross_held(lay, held):
    spots = [0]
    step = lay.head // 2
    while step:
        sent = jnp.stack([x for d in range(step) for x in held[d + step]])
        got = lay.to_plane(sent, step)
        many = len(held[0])
        for d in range(step):
            held[d] = held[d] + [got[d * many + n] for n in range(many)]
        spots = spots + [s ^ step for s in spots]
        step //= 2
    return jnp.stack(held[0]), spots


def gather_out_weight(lay, pieces):
    crossed, spots = cross_planes(lay, pieces)
    mine = jnp.concatenate(lay.double(crossed[None]), axis=0)
    both = jnp.stack([lay.to_mate(mine, m) for m in range(lay.mates)])
    columns = []
    for m in range(lay.mates):
        half = pick(both, lay.mate ^ m)
        slots = []
        for g in range(lay.groups):
            distance = lay.group ^ g
            slot = sum(
                jnp.where(lay.mask(j, jnp.int32(m)) == distance, j, 0)
                for j in range(lay.groups)
            )
            slots.append(pick(half, slot))
        columns.append(jnp.concatenate(slots, axis=1))
    return jnp.concatenate(columns, axis=2), spots


def project_text(lay, texts, key_weight, value_weight, key_gain, total_att):
    att = key_weight.shape[1]
    pair = jnp.concatenate([key_weight, value_weight], axis=1)
    weights = jnp.concatenate([lay.to_mate(pair, m) for m in range(lay.mates)], axis=0)
    partial = dot32(texts, weights)
    local = texts.shape[0] // lay.groups
    total = partial[:local]
    for k in range(1, lay.groups):
        total = total + lay.to_peer(partial[k * local : (k + 1) * local], k)
    keys, values = total[:, :att], total[:, att:]
    square = lay.plane_sum(jnp.sum(keys * keys, axis=1))
    keys = (keys / jnp.sqrt(square[:, None] / total_att + 1e-06) * key_gain).astype(
        jnp.bfloat16
    )
    packed = jnp.concatenate([keys, values.astype(jnp.bfloat16)], axis=1)
    packed = jnp.concatenate([lay.to_peer(packed, k) for k in range(lay.groups)], axis=0)
    packed = jnp.concatenate([lay.to_mate(packed, m) for m in range(lay.mates)], axis=0)
    places = jnp.concatenate(
        [
            ((lay.group ^ k) * lay.mates + (lay.mate ^ m)) * local
            + jnp.arange(local, dtype=jnp.int32)
            for m in range(lay.mates)
            for k in range(lay.groups)
        ]
    )
    return packed, places


def project_queries(lay, video_rows, query_weight):
    order = jnp.stack(
        [
            (lay.group ^ lay.mask(j, lay.mate ^ m)) * lay.mates + (lay.mate ^ m)
            for m in range(lay.mates)
            for j in range(lay.groups)
        ]
    ).astype(jnp.int32)
    normed = ordered_norm(video_rows, order)
    mine = jnp.concatenate(lay.double(query_weight), axis=0)
    depth = mine.shape[0]
    queries = None
    for m in range(lay.mates):
        term = dot32(normed[:, m * depth : (m + 1) * depth], lay.to_mate(mine, m))
        queries = term if queries is None else queries + term
    return queries, lay.plane_sum(jnp.sum(queries * queries, axis=1))


def spread_planes(lay, attended):
    have = {0: attended}
    step = lay.head // 2
    while step:
        for d in sorted(have):
            have[d ^ step] = lay.to_plane(have[d], step)
        step //= 2
    return have


def shift_and_scale(timestep, time_weight, modulation):
    half = FREQ // 2
    freqs = jnp.exp(-jnp.log(10000.0) * jnp.arange(half, dtype=jnp.float32) / half)
    angles = timestep[0].astype(jnp.float32) * freqs
    embedding = jnp.concatenate([jnp.cos(angles), jnp.sin(angles)])
    act = jax.nn.silu(embedding).astype(jnp.bfloat16)[None, :]
    shift = modulation[0] + dot32(act, time_weight[0])[0]
    scale = modulation[1] + dot32(act, time_weight[1])[0]
    return shift, scale


def on_device(
    video_rows,
    context,
    valid_length,
    timestep,
    query_weight,
    key_weight,
    value_weight,
    out_weight,
    query_gain,
    key_gain,
    time_weight,
    modulation,
):
    lay = Layout()
    if query_weight.shape[0] % 128 == 0 and out_weight.shape[0] == lay.groups * context.shape[0]:
        return aligned_path(
            lay,
            video_rows,
            context,
            valid_length,
            timestep,
            query_weight,
            key_weight,
            value_weight,
            out_weight,
            query_gain,
            key_gain,
            time_weight,
            modulation,
        )
    total_att = query_weight.shape[1] * lay.head
    width_local = modulation.shape[1]
    texts, pieces = first_exchange(lay, context, out_weight, key_weight.shape[0])
    text, places = project_text(lay, texts, key_weight, value_weight, key_gain, total_att)
    queries, square = project_queries(lay, video_rows, query_weight)
    block_rows, spots = gather_out_weight(lay, pieces)
    attended = attend(
        queries, square[:, None], query_gain, text, places, valid_length, total_att
    )
    spread = spread_planes(lay, attended)
    projected = None
    for n, d in enumerate(spots):
        term = dot32(spread[d], block_rows[n])
        projected = term if projected is None else projected + term
    video_part = take(video_rows, lay.plane, width_local, 1)
    residual_out = (video_part.astype(jnp.float32) + projected).astype(jnp.bfloat16)
    shift, scale = shift_and_scale(timestep, time_weight, modulation)
    resid = residual_out.astype(jnp.float32)
    sums = lay.plane_sum(jnp.stack([jnp.sum(resid, axis=1), jnp.sum(resid * resid, axis=1)]))
    full_width = width_local * lay.head
    mean2 = (sums[0] / full_width)[:, None]
    var2 = (sums[1] / full_width)[:, None] - mean2 * mean2
    modulated = ((resid - mean2) / jnp.sqrt(var2 + 1e-06) * (1.0 + scale) + shift).astype(
        jnp.bfloat16
    )
    return (residual_out, modulated)


def solution(mesh):
    in_specs = (
        P("seq", None),
        P("seq", None),
        P(),
        P(),
        P("seq", "head"),
        P("seq", "head"),
        P("seq", "head"),
        P("head", "seq"),
        P("head"),
        P("head"),
        P(None, None, "head"),
        P(None, "head"),
    )
    out_specs = (P("seq", "head"), P("seq", "head"))
    return jax.shard_map(
        on_device, mesh=mesh, in_specs=in_specs, out_specs=out_specs, check_vma=False
    )
```

```python
import functools

import jax
import jax.numpy as jnp
from jax import lax
from jax.experimental import pallas as pl
from jax.experimental.pallas import tpu as pltpu
from jax.sharding import PartitionSpec as P


HD = 128
FREQ = 256


def dot32(left, right):
    return jnp.dot(left, right, preferred_element_type=jnp.float32)


def take(x, index, size, axis):
    return lax.dynamic_slice_in_dim(x, index * size, size, axis)


def pick(x, index):
    return lax.dynamic_index_in_dim(x, index, 0, False)


class Layout:
    def __init__(self):
        self.seq = lax.axis_size("seq")
        self.head = lax.axis_size("head")
        self.mates = self.seq // self.head
        self.groups = self.seq // self.mates
        self.bits = self.groups.bit_length() - 1
        index = lax.axis_index("seq")
        self.group = index // self.mates
        self.mate = index % self.mates
        self.plane = lax.axis_index("head")

    def permute(self, x, axis, pairs):
        return lax.ppermute(x, axis, pairs)

    def to_peer(self, x, k):
        if k == 0:
            return x
        pairs = [
            (g * self.mates + m, (g ^ k) * self.mates + m)
            for g in range(self.groups)
            for m in range(self.mates)
        ]
        return self.permute(x, "seq", pairs)

    def to_mate(self, x, m):
        if m == 0:
            return x
        return self.permute(x, "seq", [(i, i ^ m) for i in range(self.seq)])

    def to_plane(self, x, k):
        if k == 0:
            return x
        return self.permute(x, "head", [(i, i ^ k) for i in range(self.head)])

    def turned(self, step, m):
        return 1 << ((step + m) % self.bits)

    def double(self, x):
        have = [x]
        for step in range(self.bits):
            pairs = [
                (g * self.mates + m, (g ^ self.turned(step, m)) * self.mates + m)
                for g in range(self.groups)
                for m in range(self.mates)
            ]
            whole = jnp.concatenate(have, axis=0) if step else x
            have.append(self.permute(whole, "seq", pairs))
        return have

    def to_mate_each(self, pieces, m):
        return [self.to_mate(x, m) for x in pieces]

    def mask(self, slot, mate):
        total = jnp.int32(0)
        for m in range(self.mates):
            value = 0
            for step in range(self.bits):
                if slot >> step & 1:
                    value |= self.turned(step, m)
            total = total + jnp.where(mate == m, value, 0)
        return total

    def plane_sum(self, x):
        total = x
        for k in range(1, self.head):
            total = total + self.to_plane(x, k)
        return total


def norm_kernel(order, rows_ref, out_ref):
    width = rows_ref.shape[1]
    count = order.shape[0]
    depth = width // count
    lanes = 128
    total = jnp.zeros((rows_ref.shape[0], lanes), jnp.float32)
    for c in range(width // lanes):
        total = total + rows_ref[:, c * lanes : (c + 1) * lanes].astype(jnp.float32)
    mean = jnp.sum(total, axis=-1, keepdims=True) / width
    total = jnp.zeros((rows_ref.shape[0], lanes), jnp.float32)
    for c in range(width // lanes):
        shifted = rows_ref[:, c * lanes : (c + 1) * lanes].astype(jnp.float32) - mean
        total = total + shifted * shifted
    spread = jnp.sum(total, axis=-1, keepdims=True) / width
    inverse = 1.0 / jnp.sqrt(spread + 1e-06)
    for j in range(count):
        start = pl.multiple_of(order[j] * depth, 128)
        part = rows_ref[:, pl.ds(start, depth)].astype(jnp.float32)
        out_ref[:, j * depth : (j + 1) * depth] = ((part - mean) * inverse).astype(jnp.bfloat16)


def ordered_norm(video_rows, order):
    rows, width = video_rows.shape
    tile = min(rows, 128)
    depth = width // order.shape[0]
    if depth % 128:
        normed = ordered_norm(video_rows, jnp.zeros((1,), jnp.int32))
        return jnp.concatenate(
            [take(normed, order[j], depth, 1) for j in range(order.shape[0])], axis=1
        )
    return pl.pallas_call(
        norm_kernel,
        grid_spec=pltpu.PrefetchScalarGridSpec(
            num_scalar_prefetch=1,
            grid=(rows // tile,),
            in_specs=[pl.BlockSpec((tile, width), lambda i, order: (i, 0))],
            out_specs=pl.BlockSpec((tile, width), lambda i, order: (i, 0)),
        ),
        out_shape=jax.ShapeDtypeStruct((rows, width), jnp.bfloat16),
        cost_estimate=pl.CostEstimate(
            flops=20 * rows * width, bytes_accessed=4 * rows * width, transcendentals=0
        ),
        name="ordered_norm",
    )(order, video_rows)


def attend_kernel(
    total_att, valid, queries_ref, square_ref, gain_ref, text_ref, places_ref, out_ref
):
    att = queries_ref.shape[1]
    root = jnp.sqrt(square_ref[...] / total_att + 1e-06)
    queries = (queries_ref[...] * (1.0 / root) * gain_ref[...]).astype(jnp.bfloat16)
    real = places_ref[...] < valid[0]
    for h in range(att // HD):
        own = slice(h * HD, (h + 1) * HD)
        keys = text_ref[:, own]
        values = text_ref[:, att + h * HD : att + (h + 1) * HD]
        scores = lax.dot_general(
            queries[:, own], keys, (((1,), (1,)), ((), ())), preferred_element_type=jnp.float32
        ) * HD ** (-0.5)
        scores = jnp.where(real, scores, jnp.float32(-1e30))
        shifted = jnp.exp(scores - jnp.max(scores, axis=-1, keepdims=True))
        inverse = 1.0 / jnp.sum(shifted, axis=-1, keepdims=True)
        weights = (shifted * inverse).astype(jnp.bfloat16)
        out_ref[:, own] = jnp.dot(weights, values, preferred_element_type=jnp.float32).astype(
            jnp.bfloat16
        )


def attend(queries, square, query_gain, text, places, valid_length, total_att):
    rows, att = queries.shape
    texts = text.shape[0]
    tile = min(rows, 256)
    return pl.pallas_call(
        functools.partial(attend_kernel, total_att),
        grid_spec=pltpu.PrefetchScalarGridSpec(
            num_scalar_prefetch=1,
            grid=(rows // tile,),
            in_specs=[
                pl.BlockSpec((tile, att), lambda i, v: (i, 0)),
                pl.BlockSpec((tile, 1), lambda i, v: (i, 0)),
                pl.BlockSpec((1, att), lambda i, v: (0, 0)),
                pl.BlockSpec((texts, 2 * att), lambda i, v: (0, 0)),
                pl.BlockSpec((1, texts), lambda i, v: (0, 0)),
            ],
            out_specs=pl.BlockSpec((tile, att), lambda i, v: (i, 0)),
        ),
        out_shape=jax.ShapeDtypeStruct((rows, att), jnp.bfloat16),
        cost_estimate=pl.CostEstimate(
            flops=4 * rows * att * texts,
            bytes_accessed=6 * rows * att + 4 * texts * att,
            transcendentals=rows * texts * att // HD,
        ),
        name="attend",
    )(valid_length, queries, square, query_gain[None, :], text, places[None, :])


VMEM = pl.BlockSpec(memory_space=pltpu.VMEM)
HBM = pl.BlockSpec(memory_space=pltpu.HBM)
SMEM = pl.BlockSpec(memory_space=pltpu.SMEM)


def call(kernel, outs, *args, flops=0, limit=24, specs=None, outs_at=None, scratch=()):
    moved = sum(a.size * a.dtype.itemsize for a in args)
    moved += sum(o.size * o.dtype.itemsize for o in outs)
    return pl.pallas_call(
        kernel,
        out_shape=outs,
        in_specs=specs or [VMEM] * len(args),
        out_specs=outs_at or [VMEM] * len(outs),
        scratch_shapes=scratch,
        compiler_params=pltpu.CompilerParams(vmem_limit_bytes=int(limit * 2**20)),
        cost_estimate=pl.CostEstimate(flops=flops, bytes_accessed=moved, transcendentals=0),
    )(*args)


def shape(*dims, dtype=jnp.bfloat16):
    return jax.ShapeDtypeStruct(dims, dtype)


def pack_kernel(context_hbm, weight_hbm, *refs):
    lay = Layout()
    out_refs, (context_ref, weight_ref, sems) = refs[: lay.groups], refs[lay.groups :]
    copies = [
        pltpu.make_async_copy(context_hbm, context_ref, sems.at[0]),
        pltpu.make_async_copy(weight_hbm, weight_ref, sems.at[1]),
    ]
    for copy in copies:
        copy.start()
    for copy in copies:
        copy.wait()
    piece = weight_ref.shape[0] // lay.groups
    depth = context_ref.shape[1] // lay.seq
    for k, out_ref in enumerate(out_refs):
        group = lay.group ^ k
        for m in range(lay.mates):
            start = pl.multiple_of((group * lay.mates + (lay.mate ^ m)) * depth, 128)
            out_ref[:, m * depth : (m + 1) * depth] = context_ref[:, pl.ds(start, depth)]
        start = pl.multiple_of(group * piece, 16)
        out_ref[:, lay.mates * depth :] = weight_ref[pl.ds(start, piece), :]


def rows_norm_kernel(source_ref, out_ref, rows_ref, sems):
    lay = Layout()
    rows, width = rows_ref.shape
    parts = sems.shape[0]
    many = rows // parts
    copies = [
        pltpu.make_async_copy(
            source_ref.at[n * many : (n + 1) * many],
            rows_ref.at[n * many : (n + 1) * many],
            sems.at[n],
        )
        for n in range(parts)
    ]
    for copy in copies:
        copy.start()
    depth = width // lay.seq
    lanes, tile = 128, 32
    starts = [
        pl.multiple_of(
            ((lay.group ^ lay.mask(j, lay.mate ^ m)) * lay.mates + (lay.mate ^ m)) * depth, 128
        )
        for m in range(lay.mates)
        for j in range(lay.groups)
    ]

    def norm_tile(i):
        here = pl.ds(pl.multiple_of(i * tile, tile), tile)

        def part(c):
            return rows_ref[here, c * lanes : (c + 1) * lanes].astype(jnp.float32)

        sums = [jnp.zeros((tile, lanes), jnp.float32) for _ in range(4)]
        for c in range(width // lanes):
            sums[c % 4] = sums[c % 4] + part(c)
        mean = jnp.sum(sum(sums[1:], sums[0]), axis=-1, keepdims=True) / width
        mean = jnp.broadcast_to(mean, (tile, lanes))
        sums = [jnp.zeros((tile, lanes), jnp.float32) for _ in range(4)]
        for c in range(width // lanes):
            shifted = part(c) - mean
            sums[c % 4] = sums[c % 4] + shifted * shifted
        spread = jnp.sum(sum(sums[1:], sums[0]), axis=-1, keepdims=True) / width
        inverse = jnp.broadcast_to(1.0 / jnp.sqrt(spread + 1e-06), (tile, lanes))
        for j, start in enumerate(starts):
            for c in range(depth // lanes):
                source = pl.ds(pl.multiple_of(start + c * lanes, lanes), lanes)
                target = slice(j * depth + c * lanes, j * depth + (c + 1) * lanes)
                values = rows_ref[here, source].astype(jnp.float32)
                out_ref[here, target] = ((values - mean) * inverse).astype(jnp.bfloat16)

    for n, copy in enumerate(copies):
        copy.wait()
        pl.loop(n * many // tile, (n + 1) * many // tile)(norm_tile)


def text_kernel(depth, *refs):
    lay = Layout()
    got, refs = refs[: lay.groups], refs[lay.groups :]
    keys, refs = refs[: lay.mates], refs[lay.mates :]
    values, refs = refs[: lay.mates], refs[lay.mates :]
    totals, pieces_ref = refs[: lay.groups], refs[lay.groups]
    att = keys[0].shape[1]
    local = got[0].shape[0]
    rows = [
        jnp.concatenate([g[:, m * depth : (m + 1) * depth] for g in got], axis=0)
        for m in range(lay.mates)
    ]
    for at, weights in ((0, keys), (att, values)):
        total = dot32(rows[0], weights[0][...])
        for m in range(1, lay.mates):
            total = total + dot32(rows[m], weights[m][...])
        for k in range(lay.groups):
            totals[k][:, at : at + att] = total[k * local : (k + 1) * local]
    for k in range(lay.groups):
        spot = lay.group ^ lay.plane ^ k
        pieces_ref[pl.ds(spot, 1)] = got[k][:, lay.mates * depth :][None]


def to_row(column):
    return jnp.transpose(jnp.broadcast_to(column, (column.shape[0], 128)))[:1]


def to_column(row):
    wide = jnp.broadcast_to(row, (128, row.shape[1]))
    return jnp.transpose(wide)[:, :1]


def products(normed_ref, here, weights, offsets):
    total = None
    for weight_ref, at in zip(weights, offsets):
        depth = weight_ref.shape[0]
        term = dot32(normed_ref[here, at : at + depth], weight_ref[...])
        total = term if total is None else total + term
    return total


def early_kernel(offsets, normed_ref, *refs):
    weights, out_ref = refs[:-1], refs[-1]
    rows = normed_ref.shape[0]
    tile = min(rows, 256)
    for t in range(rows // tile):
        here = slice(t * tile, (t + 1) * tile)
        out_ref[here] = products(normed_ref, here, weights, offsets)


def queries_kernel(offsets, normed_ref, early_ref, *refs):
    weights, (out_ref, square_ref) = refs[:-2], refs[-2:]
    rows = normed_ref.shape[0]
    tile = min(rows, 256)
    for t in range(rows // tile):
        here = slice(t * tile, (t + 1) * tile)
        total = early_ref[here] + products(normed_ref, here, weights, offsets)
        out_ref[here] = total
        square_ref[:, here] = to_row(jnp.sum(total * total, axis=1, keepdims=True))


def scale_kernel(total_att, local, valid_ref, queries_ref, square_ref, gain_ref, out_ref, real_ref):
    lay = Layout()
    rows = queries_ref.shape[0]
    tile = min(rows, 128)
    for i in range(rows // tile):
        here = slice(i * tile, (i + 1) * tile)
        root = jnp.sqrt(to_column(square_ref[:, here]) / total_att + 1e-06)
        out_ref[here] = (queries_ref[here] * (1.0 / root) * gain_ref[...]).astype(jnp.bfloat16)
    count = local * lay.groups
    column = lax.broadcasted_iota(jnp.int32, (1, count), 1)
    for m in range(lay.mates):
        place = column % local
        for k in range(lay.groups):
            base = ((lay.group ^ k) * lay.mates + (lay.mate ^ m)) * local
            place = place + jnp.where(column // local == k, base, 0)
        real_ref[:, m * count : (m + 1) * count] = (place < valid_ref[0]).astype(jnp.float32)


def head_kernel(head, queries_ref, real_ref, *refs):
    texts, out_ref = refs[:-1], refs[-1]
    rows, att = queries_ref.shape
    tile = min(rows, 512)
    own = slice(head * HD, (head + 1) * HD)
    at = slice(att + head * HD, att + (head + 1) * HD)
    keys = jnp.concatenate([t[:, own] for t in texts], axis=0)
    values = jnp.concatenate([t[:, at] for t in texts], axis=0)
    real = real_ref[...] > 0.0
    for i in range(rows // tile):
        here = slice(i * tile, (i + 1) * tile)
        scores = lax.dot_general(
            queries_ref[here, own],
            keys,
            (((1,), (1,)), ((), ())),
            preferred_element_type=jnp.float32,
        ) * HD ** (-0.5)
        scores = jnp.where(real, scores, jnp.float32(-1e30))
        shifted = jnp.exp(scores - jnp.max(scores, axis=-1, keepdims=True))
        inverse = 1.0 / jnp.sum(shifted, axis=-1, keepdims=True)
        weights = (shifted * inverse).astype(jnp.bfloat16)
        out_ref[here] = dot32(weights, values).astype(jnp.bfloat16)


def place_kernel(*refs):
    lay = Layout()
    pieces, out_ref = refs[:-1], refs[-1]
    piece, cols = pieces[0].shape[2:]
    each = len(pieces) // lay.mates
    for m in range(lay.mates):
        at = pl.multiple_of((lay.mate ^ m) * cols, 128)
        j = 0
        for ref in pieces[m * each : (m + 1) * each]:
            for n in range(ref.shape[0]):
                row = pl.multiple_of((lay.group ^ lay.mask(j, lay.mate ^ m)) * piece, 16)
                out_ref[:, pl.ds(row, piece), pl.ds(at, cols)] = ref[n]
                j += 1


def side_by_side(pieces, here):
    return jnp.concatenate([p[here] for p in pieces], axis=1)


def most_kernel(count, heads, *refs):
    lay = Layout()
    weight_ref, video_ref, out_ref, part_ref, sem = refs[-5:]
    rows, width = out_ref.shape
    start = pl.multiple_of(lay.plane * width, 128)
    copy = pltpu.make_async_copy(video_ref.at[:, pl.ds(start, width)], part_ref, sem)
    copy.start()
    tile = min(rows, 128)
    for i in range(rows // tile):
        here = slice(i * tile, (i + 1) * tile)
        total = None
        for n in range(count):
            left = side_by_side(refs[n * heads : (n + 1) * heads], here)
            term = dot32(left, weight_ref[n])
            total = term if total is None else total + term
        if i == 0:
            copy.wait()
        out_ref[here] = total + part_ref[here].astype(jnp.float32)


def last_kernel(last, heads, *refs):
    pieces, (partial_ref, weight_ref, out_ref, sums_ref) = refs[:heads], refs[heads:]
    rows = out_ref.shape[0]
    tile = min(rows, 128)
    for i in range(rows // tile):
        here = slice(i * tile, (i + 1) * tile)
        total = partial_ref[here] + dot32(side_by_side(pieces, here), weight_ref[last])
        resid = total.astype(jnp.bfloat16)
        out_ref[here] = resid
        resid = resid.astype(jnp.float32)
        sums_ref[0:1, here] = to_row(jnp.sum(resid, axis=1, keepdims=True))
        sums_ref[1:2, here] = to_row(jnp.sum(resid * resid, axis=1, keepdims=True))


def modulate_kernel(
    full_width, resid_ref, sums_ref, shift_ref, scale_ref, first_ref, out_ref, tiles_ref, sems
):
    rows = resid_ref.shape[0]
    tile = min(rows, 128)
    copies = [pltpu.make_async_copy(resid_ref, first_ref, sems.at[0])]
    copies[0].start()
    for i in range(rows // tile):
        here = slice(i * tile, (i + 1) * tile)
        mean = to_column(sums_ref[0:1, here]) / full_width
        square = to_column(sums_ref[1:2, here]) / full_width
        inverse = 1.0 / jnp.sqrt(square - mean * mean + 1e-06)
        resid = resid_ref[here].astype(jnp.float32)
        tiles_ref[here] = (
            (resid - mean) * inverse * (1.0 + scale_ref[...]) + shift_ref[...]
        ).astype(jnp.bfloat16)
        copies.append(
            pltpu.make_async_copy(tiles_ref.at[here], out_ref.at[here], sems.at[i + 1])
        )
        copies[-1].start()
    for copy in copies:
        copy.wait()


def aligned_path(
    lay,
    video_rows,
    context,
    valid_length,
    timestep,
    query_weight,
    key_weight,
    value_weight,
    out_weight,
    query_gain,
    key_gain,
    time_weight,
    modulation,
):
    f32 = jnp.float32
    rows, width = video_rows.shape
    local = context.shape[0]
    depth, att = key_weight.shape
    piece, cols = out_weight.shape[0] // lay.groups, out_weight.shape[1]
    width_local = modulation.shape[1]
    total_att = att * lay.head

    packed = lay.mates * depth + cols
    sent = call(
        pack_kernel,
        [shape(local, packed)] * lay.groups,
        context,
        out_weight,
        specs=[HBM] * 2,
        limit=62.65,
        scratch=[
            pltpu.VMEM(context.shape, jnp.bfloat16),
            pltpu.VMEM(out_weight.shape, jnp.bfloat16),
            pltpu.SemaphoreType.DMA((2,)),
        ],
    )
    got = [lay.to_peer(x, k) for k, x in enumerate(sent)]
    key_parts = [lay.to_mate(key_weight, m) for m in range(lay.mates)]
    value_parts = [lay.to_mate(value_weight, m) for m in range(lay.mates)]
    (normed,) = call(
        rows_norm_kernel,
        [shape(rows, width)],
        video_rows,
        flops=40 * rows * width,
        specs=[HBM],
        scratch=[pltpu.VMEM((rows, width), jnp.bfloat16), pltpu.SemaphoreType.DMA((4,))],
    )
    mine = lay.double(query_weight)
    *totals, pieces = call(
        functools.partial(text_kernel, depth),
        [shape(local, 2 * att, dtype=f32)] * lay.groups + [shape(lay.head, piece, cols)],
        *got,
        *key_parts,
        *value_parts,
        flops=4 * local * lay.groups * lay.mates * depth * att,
    )
    total = totals[0]
    for k in range(1, lay.groups):
        total = total + lay.to_peer(totals[k], k)
    keys, values = total[:, :att], total[:, att:]
    pieces_in, offsets, at = [], [], 0
    for m in range(lay.mates):
        for piece_in in lay.to_mate_each(mine, m):
            pieces_in.append(piece_in)
            offsets.append(at)
            at += piece_in.shape[0]
    late = [n for n in range(len(pieces_in)) if (n + 1) % len(mine) == 0]
    soon = [n for n in range(len(pieces_in)) if n not in late]
    (early,) = call(
        functools.partial(early_kernel, [offsets[n] for n in soon]),
        [shape(rows, att, dtype=f32)],
        normed,
        *[pieces_in[n] for n in soon],
        flops=rows * width * att,
    )
    queries, square = call(
        functools.partial(queries_kernel, [offsets[n] for n in late]),
        [shape(rows, att, dtype=f32), shape(1, rows, dtype=f32)],
        normed,
        early,
        *[pieces_in[n] for n in late],
        flops=rows * width * att,
    )
    square = jnp.concatenate([square, jnp.sum(keys * keys, axis=1)[None, :]], axis=1)
    square = lay.plane_sum(square)
    key_square, square = square[0, rows:, None], square[:, :rows]
    keys = (keys / jnp.sqrt(key_square / total_att + 1e-06) * key_gain).astype(jnp.bfloat16)
    text = jnp.concatenate([keys, values.astype(jnp.bfloat16)], axis=1)
    text = jnp.concatenate([lay.to_peer(text, k) for k in range(lay.groups)], axis=0)
    texts = [lay.to_mate(text, m) for m in range(lay.mates)]

    held = {d: [pieces[d]] for d in range(lay.head)}
    crossed, spots = cross_held(lay, held)
    mine = lay.double(crossed[None])
    (weights,) = call(
        place_kernel,
        [shape(lay.head, out_weight.shape[0], width_local)],
        *[x for m in range(lay.mates) for x in lay.to_mate_each(mine, m)],
        flops=width_local * width,
    )

    queries, real = call(
        functools.partial(scale_kernel, total_att, local),
        [shape(rows, att), shape(1, local * lay.seq, dtype=f32)],
        valid_length,
        queries,
        square,
        query_gain[None, :],
        flops=8 * rows * att,
        specs=[SMEM] + [VMEM] * 3,
    )
    heads = att // HD
    spread = []
    for h in range(heads):
        (attended,) = call(
            functools.partial(head_kernel, h),
            [shape(rows, HD)],
            queries,
            real,
            *texts,
            flops=8 * rows * HD * local * lay.seq,
        )
        spread.append(spread_planes(lay, attended))
    most = lay.head - 1
    (partial,) = call(
        functools.partial(most_kernel, most, heads),
        [shape(rows, width_local, dtype=f32)],
        *[spread[h][d] for d in spots[:-1] for h in range(heads)],
        weights,
        video_rows,
        flops=2 * most * rows * att * width_local,
        specs=[VMEM] * (most * heads + 1) + [HBM],
        scratch=[pltpu.VMEM((rows, width_local), jnp.bfloat16), pltpu.SemaphoreType.DMA],
    )
    resid, sums = call(
        functools.partial(last_kernel, most, heads),
        [shape(rows, width_local), shape(2, rows, dtype=f32)],
        *[spread[h][spots[-1]] for h in range(heads)],
        partial,
        weights,
        flops=2 * rows * att * width_local,
    )
    sums = lay.plane_sum(sums)
    shift, scale = shift_and_scale(timestep, time_weight, modulation)
    residual_out, modulated = call(
        functools.partial(modulate_kernel, width_local * lay.head),
        [shape(rows, width_local)] * 2,
        resid,
        sums,
        shift[None, :],
        scale[None, :],
        flops=8 * rows * width_local,
        outs_at=[HBM] * 2,
        scratch=[pltpu.VMEM((rows, width_local), jnp.bfloat16), pltpu.SemaphoreType.DMA((8,))],
    )
    return residual_out, modulated


def first_exchange(lay, context, out_weight, depth):
    piece = out_weight.shape[0] // lay.groups
    text_local = context.shape[0]
    texts, pieces = [], []
    for k in range(lay.groups):
        columns = [
            take(context, (lay.group ^ k) * lay.mates + (lay.mate ^ m), depth, 1)
            for m in range(lay.mates)
        ]
        rows = take(out_weight, lay.group ^ k, piece, 0).reshape(text_local, -1)
        both = lay.to_peer(jnp.concatenate(columns + [rows], axis=1), k)
        texts.append(both[:, : lay.mates * depth])
        pieces.append(both[:, lay.mates * depth :].reshape(piece, -1))
    return jnp.concatenate(texts, axis=0), jnp.stack(pieces)


def cross_planes(lay, pieces):
    held = {d: [pick(pieces, lay.group ^ lay.plane ^ d)] for d in range(lay.head)}
    return cross_held(lay, held)


def cross_held(lay, held):
    spots = [0]
    step = lay.head // 2
    while step:
        sent = jnp.stack([x for d in range(step) for x in held[d + step]])
        got = lay.to_plane(sent, step)
        many = len(held[0])
        for d in range(step):
            held[d] = held[d] + [got[d * many + n] for n in range(many)]
        spots = spots + [s ^ step for s in spots]
        step //= 2
    return jnp.stack(held[0]), spots


def gather_out_weight(lay, pieces):
    crossed, spots = cross_planes(lay, pieces)
    mine = jnp.concatenate(lay.double(crossed[None]), axis=0)
    both = jnp.stack([lay.to_mate(mine, m) for m in range(lay.mates)])
    columns = []
    for m in range(lay.mates):
        half = pick(both, lay.mate ^ m)
        slots = []
        for g in range(lay.groups):
            distance = lay.group ^ g
            slot = sum(
                jnp.where(lay.mask(j, jnp.int32(m)) == distance, j, 0)
                for j in range(lay.groups)
            )
            slots.append(pick(half, slot))
        columns.append(jnp.concatenate(slots, axis=1))
    return jnp.concatenate(columns, axis=2), spots


def project_text(lay, texts, key_weight, value_weight, key_gain, total_att):
    att = key_weight.shape[1]
    pair = jnp.concatenate([key_weight, value_weight], axis=1)
    weights = jnp.concatenate([lay.to_mate(pair, m) for m in range(lay.mates)], axis=0)
    partial = dot32(texts, weights)
    local = texts.shape[0] // lay.groups
    total = partial[:local]
    for k in range(1, lay.groups):
        total = total + lay.to_peer(partial[k * local : (k + 1) * local], k)
    keys, values = total[:, :att], total[:, att:]
    square = lay.plane_sum(jnp.sum(keys * keys, axis=1))
    keys = (keys / jnp.sqrt(square[:, None] / total_att + 1e-06) * key_gain).astype(
        jnp.bfloat16
    )
    packed = jnp.concatenate([keys, values.astype(jnp.bfloat16)], axis=1)
    packed = jnp.concatenate([lay.to_peer(packed, k) for k in range(lay.groups)], axis=0)
    packed = jnp.concatenate([lay.to_mate(packed, m) for m in range(lay.mates)], axis=0)
    places = jnp.concatenate(
        [
            ((lay.group ^ k) * lay.mates + (lay.mate ^ m)) * local
            + jnp.arange(local, dtype=jnp.int32)
            for m in range(lay.mates)
            for k in range(lay.groups)
        ]
    )
    return packed, places


def project_queries(lay, video_rows, query_weight):
    order = jnp.stack(
        [
            (lay.group ^ lay.mask(j, lay.mate ^ m)) * lay.mates + (lay.mate ^ m)
            for m in range(lay.mates)
            for j in range(lay.groups)
        ]
    ).astype(jnp.int32)
    normed = ordered_norm(video_rows, order)
    mine = jnp.concatenate(lay.double(query_weight), axis=0)
    depth = mine.shape[0]
    queries = None
    for m in range(lay.mates):
        term = dot32(normed[:, m * depth : (m + 1) * depth], lay.to_mate(mine, m))
        queries = term if queries is None else queries + term
    return queries, lay.plane_sum(jnp.sum(queries * queries, axis=1))


def spread_planes(lay, attended):
    have = {0: attended}
    step = lay.head // 2
    while step:
        for d in sorted(have):
            have[d ^ step] = lay.to_plane(have[d], step)
        step //= 2
    return have


def shift_and_scale(timestep, time_weight, modulation):
    half = FREQ // 2
    freqs = jnp.exp(-jnp.log(10000.0) * jnp.arange(half, dtype=jnp.float32) / half)
    angles = timestep[0].astype(jnp.float32) * freqs
    embedding = jnp.concatenate([jnp.cos(angles), jnp.sin(angles)])
    act = jax.nn.silu(embedding).astype(jnp.bfloat16)[None, :]
    shift = modulation[0] + dot32(act, time_weight[0])[0]
    scale = modulation[1] + dot32(act, time_weight[1])[0]
    return shift, scale


def on_device(
    video_rows,
    context,
    valid_length,
    timestep,
    query_weight,
    key_weight,
    value_weight,
    out_weight,
    query_gain,
    key_gain,
    time_weight,
    modulation,
):
    lay = Layout()
    if query_weight.shape[0] % 128 == 0 and out_weight.shape[0] == lay.groups * context.shape[0]:
        return aligned_path(
            lay,
            video_rows,
            context,
            valid_length,
            timestep,
            query_weight,
            key_weight,
            value_weight,
            out_weight,
            query_gain,
            key_gain,
            time_weight,
            modulation,
        )
    total_att = query_weight.shape[1] * lay.head
    width_local = modulation.shape[1]
    texts, pieces = first_exchange(lay, context, out_weight, key_weight.shape[0])
    text, places = project_text(lay, texts, key_weight, value_weight, key_gain, total_att)
    queries, square = project_queries(lay, video_rows, query_weight)
    block_rows, spots = gather_out_weight(lay, pieces)
    attended = attend(
        queries, square[:, None], query_gain, text, places, valid_length, total_att
    )
    spread = spread_planes(lay, attended)
    projected = None
    for n, d in enumerate(spots):
        term = dot32(spread[d], block_rows[n])
        projected = term if projected is None else projected + term
    video_part = take(video_rows, lay.plane, width_local, 1)
    residual_out = (video_part.astype(jnp.float32) + projected).astype(jnp.bfloat16)
    shift, scale = shift_and_scale(timestep, time_weight, modulation)
    resid = residual_out.astype(jnp.float32)
    sums = lay.plane_sum(jnp.stack([jnp.sum(resid, axis=1), jnp.sum(resid * resid, axis=1)]))
    full_width = width_local * lay.head
    mean2 = (sums[0] / full_width)[:, None]
    var2 = (sums[1] / full_width)[:, None] - mean2 * mean2
    modulated = ((resid - mean2) / jnp.sqrt(var2 + 1e-06) * (1.0 + scale) + shift).astype(
        jnp.bfloat16
    )
    return (residual_out, modulated)


def solution(mesh):
    in_specs = (
        P("seq", None),
        P("seq", None),
        P(),
        P(),
        P("seq", "head"),
        P("seq", "head"),
        P("seq", "head"),
        P("head", "seq"),
        P("head"),
        P("head"),
        P(None, None, "head"),
        P(None, "head"),
    )
    out_specs = (P("seq", "head"), P("seq", "head"))
    return jax.shard_map(
        on_device, mesh=mesh, in_specs=in_specs, out_specs=out_specs, check_vma=False
    )
```
